256 devices in a mesh: tm: 64 (over x, z, core), env: 4 (over y).
Axes of the slice: x: 4, y: 4, z: 8, core: 2. Of those that a mesh axis runs over, the one named last changes fastest.
Arguments:
- init_state: float32 [70, 1024], P(None, 'env'), may hold values from -6 to 6
- torque: float32 [256, 35, 1024], P('tm', None, 'env'), may hold values from -192 to 192
- contact: int32 [256, 1024], P('tm', 'env'), may hold values 0 or 1
- mass_inverse: float32 [128, 35, 35], P('tm'), may hold values from -0.014 to 1.5, as said below
- stiffness: float32 [35], replicated, may hold values from 10 to 100
- damping: float32 [35], replicated, may hold values from 0.5 to 5
- gravity: float32 [35], replicated, may hold values from 1 to 10
- contact_stiffness: float32 [35], replicated, may hold values from 20 to 100
- contact_damping: float32 [35], replicated, may hold values from 0.5 to 3
Outputs:
- final_states: float32 [128, 70, 1024], P('tm', None, 'env')
- corrections: float32 [3, 1024], P(None, 'env')
The draws below stay inside these ranges and needn't reach their ends.
Inputs may be any that keep to these rules, and one draw needn't show every extreme that they name: `mass_inverse`: each matrix is symmetric, and each diagonal entry exceeds the sum of the magnitudes of the other entries of its row.
All inputs are finite; a program needn't handle non-finite values. No bound on the sum of `contact` on one device may be relied on, other than what follows from the above.
Results may differ from the reference program's by a relative error of at most 0.00025.
Values sent between devices are 32-bit elements; how exact they have to be, the bound alone decides.
A program may use at most 64 MiB of HBM per device.

```python
import math
import jax
import jax.numpy as jnp
from jax import lax

DOF = 35
STATE = 70
HS = 2
SUB = 32
ITERS = 3
SLICES = 128
STEPS = 256
ENV = 1024


def draw_mass_inverse(key, part):
    key_diag = jax.random.fold_in(key, 11)
    key_off = jax.random.fold_in(key, 12)
    diagonal = jax.random.uniform(key_diag, (SLICES, DOF), jnp.float32, 0.5, 1.5)
    raw = jnp.clip(0.008 * jax.random.normal(key_off, (SLICES, DOF, DOF), jnp.float32), -0.014, 0.014)
    upper = jnp.triu(raw, 1)
    return upper + jnp.swapaxes(upper, 1, 2) + diagonal[:, :, None] * jnp.eye(DOF, dtype=jnp.float32)


def touch_ends(values, own_key, low, largest):
    spot = [jax.random.randint(jax.random.fold_in(own_key, axis), (), 0, length) for axis, length in enumerate(values.shape)]
    widest = values.shape.index(max(values.shape))
    neighbour = spot[:widest] + [(spot[widest] + 1) % values.shape[widest]] + spot[widest + 1:]
    return values.at[tuple(spot)].set(low).at[tuple(neighbour)].set(largest)


def shard_levels(key, extent, cuts, low, largest):
    factor_of, own = 1.0, jax.random.fold_in(key, 6)
    for position, shards_of in cuts:
        draws = jnp.exp(jax.random.uniform(jax.random.fold_in(own, position), (shards_of,), jnp.float32, low / len(cuts), largest / len(cuts)))
        factor_of = factor_of * jnp.repeat(draws, extent[position] // shards_of).reshape([-1 if axis == position else 1 for axis in range(len(extent))])
    return factor_of


def gaussian(own_key, dims, deviation, most, shards=(), kind=jnp.bfloat16):
    array = jax.random.normal(own_key, dims, jnp.float32) * deviation
    if len(shards) > 0:
        array = shard_levels(own_key, dims, shards, -0.22, 0.18) * array
    return jnp.clip(array, min=-most, max=most).astype(kind)


def setup_inputs(seed: int = 0) -> dict:
    arg_keys = jax.random.split(jax.random.key(seed), 10)
    return {
        "init_state": gaussian(arg_keys[0], (STATE, ENV), 0.5, 6.0, ((1, 4),), jnp.float32),
        "torque": gaussian(arg_keys[1], (STEPS, DOF, ENV), 30.0, 192.0, ((0, 64), (2, 4)), jnp.float32),
        "contact": touch_ends((jax.random.randint(arg_keys[2], (STEPS, ENV), 0, 3) < 1).astype(jnp.int32), jax.random.fold_in(arg_keys[2], 1), 0, 1),
        "mass_inverse": draw_mass_inverse(jax.random.fold_in(arg_keys[9], 71), 0),
        "stiffness": jnp.clip(jnp.exp(jax.random.uniform(arg_keys[4], (DOF,), jnp.float32, math.log(10.0), math.log(100.0))), 10.0, 100.0),
        "damping": jnp.clip(jnp.exp(jax.random.uniform(arg_keys[5], (DOF,), jnp.float32, math.log(0.5), math.log(5.0))), 0.5, 5.0),
        "gravity": jnp.clip(jnp.exp(jax.random.uniform(arg_keys[6], (DOF,), jnp.float32, math.log(1.0), math.log(10.0))), 1.0, 10.0),
        "contact_stiffness": jnp.clip(jnp.exp(jax.random.uniform(arg_keys[7], (DOF,), jnp.float32, math.log(20.0), math.log(100.0))), 20.0, 100.0),
        "contact_damping": jnp.clip(jnp.exp(jax.random.uniform(arg_keys[8], (DOF,), jnp.float32, math.log(0.5), math.log(3.0))), 0.5, 3.0),
    }


step_length = 0.05

def exact_dot(left, right):
    return jnp.dot(left, right, precision=lax.Precision.HIGHEST, preferred_element_type=jnp.float32)

def coarse_one(state_now, torque_steps, mean_steps, inverse, params):
    stiffness, damping, gravity, contact_stiffness, contact_damping = params
    joint_pos = state_now[:DOF]
    joint_vel = state_now[DOF:]
    for step_pos in range(HS):
        spring = (stiffness + gravity + mean_steps[step_pos] * contact_stiffness)[:, None]
        friction = (damping + mean_steps[step_pos] * contact_damping)[:, None]
        force = torque_steps[step_pos] - spring * joint_pos - friction * joint_vel
        joint_vel = joint_vel + step_length * exact_dot(inverse, force)
        joint_pos = joint_pos + step_length * joint_vel
    return jnp.concatenate([joint_pos, joint_vel], axis=0)

def fine_one(state_now, torque_steps, contact_steps, inverse, params):
    stiffness, damping, gravity, contact_stiffness, contact_damping = params
    fine_dt = step_length / SUB
    joint_pair = (state_now[:DOF], state_now[DOF:])
    for step_pos in range(HS):
        torque_here = torque_steps[step_pos]
        contact_here = contact_steps[step_pos][None, :]

        def substep(counter, pair_now):
            joint_pos, joint_vel = pair_now
            force = torque_here - stiffness[:, None] * joint_pos - damping[:, None] * joint_vel - gravity[:, None] * jnp.sin(joint_pos) - contact_here * (contact_stiffness[:, None] * joint_pos + contact_damping[:, None] * joint_vel)
            joint_vel = joint_vel + fine_dt * exact_dot(inverse, force)
            joint_pos = joint_pos + fine_dt * joint_vel
            return (joint_pos, joint_vel)
        joint_pair = lax.fori_loop(0, SUB, substep, joint_pair)
    return jnp.concatenate([joint_pair[0], joint_pair[1]], axis=0)

def reference(init_state, torque, contact, mass_inverse, stiffness, damping, gravity, contact_stiffness, contact_damping):
    params = (stiffness, damping, gravity, contact_stiffness, contact_damping)
    torque_steps = torque.reshape(SLICES, HS, DOF, ENV)
    contact_steps = contact.astype(jnp.float32).reshape(SLICES, HS, ENV)
    mean_steps = lax.optimization_barrier(jnp.mean(contact_steps, axis=2))
    coarse_all = jax.vmap(coarse_one, in_axes=(0, 0, 0, 0, None))
    fine_all = jax.vmap(fine_one, in_axes=(0, 0, 0, 0, None))

    def chain(jumps):

        def advance(state_now, inputs):
            torque_here, mean_here, inverse, jump = inputs
            following = coarse_one(state_now, torque_here, mean_here, inverse, params) + jump
            return (following, following)
        unused, ends = lax.scan(advance, init_state, (torque_steps, mean_steps, mass_inverse, jumps))
        return ends
    ends = chain(jnp.zeros((SLICES, STATE, ENV), jnp.float32))
    records = []
    for iteration in range(ITERS):
        starts = jnp.concatenate([init_state[None], ends[:-1]], axis=0)
        jumps = fine_all(starts, torque_steps, contact_steps, mass_inverse, params) - coarse_all(starts, torque_steps, mean_steps, mass_inverse, params)
        new_ends = chain(jumps)
        records.append(lax.optimization_barrier(jnp.max(jnp.sqrt(lax.optimization_barrier(jnp.sum((new_ends - ends) ** 2, axis=1))), axis=0)))
        ends = new_ends
    return (ends, jnp.stack(records))
```

```python
import math

import jax
import jax.numpy as jnp
import numpy as np
from jax import lax
from jax.experimental import pallas as pl
from jax.experimental.pallas import tpu as pltpu
from jax.sharding import Mesh
from jax.sharding import PartitionSpec as P

DOF = 35
STATE = 70
SUB = 32
ITERS = 3
SWEEPS = ITERS + 1
NX, NZ, NC, NE = 4, 8, 2, 4
GROUP = NZ * NC
ENV = 256
BLOCK = ENV // GROUP
LANES = 128
HALF = 64
ROWS = 72
DT = 0.05
H = DT / SUB
TWO_PI = 2.0 * math.pi
MAGIC = 12582912.0
F32 = jnp.float32
BF16 = jnp.bfloat16
MESH = pl.DeviceIdType.MESH
HIGHEST = lax.Precision.HIGHEST
TM = ("x", "z", "c")
Z_OFFSETS = (4, 3, 5, 2, 6, 1, 7, 0)


def sine_coefficients(terms):
    x = np.cos(np.linspace(0, np.pi, 4001)) * 0.25 + 0.25
    x = x[x > 1e-4]
    basis = np.stack([x ** (2 * i + 1) for i in range(terms)], 1)
    target = np.sin(2 * np.pi * x)
    weight = np.ones_like(x)
    for _ in range(200):
        c = np.linalg.lstsq(basis * weight[:, None], target * weight, rcond=None)[0]
        weight = weight * (1e-12 + np.abs(basis @ c - target)) ** 0.1
        weight /= weight.mean()
    return [float(np.float32(v)) for v in c]


SINE = sine_coefficients(6)


def selectors():
    pick = np.zeros((2, 2 * LANES, LANES), np.float32)
    for s in range(2):
        for i in range(DOF):
            pick[s, HALF * s + i, i] = 1.0
            pick[s, LANES + HALF * s + i, DOF + i] = 1.0
    return pick


PICK = selectors()


def split(x):
    hi = x.astype(BF16)
    lo = (x - hi.astype(F32)).astype(BF16)
    return hi, lo


def dot(a, b):
    return jnp.dot(a, b, preferred_element_type=F32)


def exact(a, b):
    return jnp.dot(a, b, precision=HIGHEST, preferred_element_type=F32)


def exact_ta(a, b):
    return lax.dot_general(a, b, (((0,), (0,)), ((), ())), precision=HIGHEST, preferred_element_type=F32)


def exact_tb(a, b):
    return lax.dot_general(a, b, (((1,), (1,)), ((), ())), precision=HIGHEST, preferred_element_type=F32)


def wide(x, weights):
    hi, lo = split(x)
    return dot(hi, weights[0]) + dot(lo, weights[0]) + dot(hi, weights[1])


def put_pair(ref, value):
    hi, lo = split(value)
    ref[0] = hi
    ref[1] = lo


def put_side(ref, index, value):
    hi, lo = split(value)
    ref[index, :, 0:LANES] = hi
    ref[index, :, LANES:] = lo


def small(x, weights):
    hi, lo = split(x)
    out = dot(jnp.concatenate([hi, lo], axis=0), weights)
    both = out[:, 0:LANES] + out[:, LANES:]
    return both[0:BLOCK] + both[BLOCK:]


def body(
    init_ref, torque_ref, contact_ref, block_ref, par_ref, pick_ref,
    final_ref, corr_out_ref,
    flip, tau, kk, dd, q_ref, v_ref, init_t, nfine, free, jall, start, gee, ends, jshift,
    mf_w, zf_w, ze_w, s_buf, recv_s, recv_a, a_buf, side_a, side_b, side_p, side_pp, side_c,
    prod, ent, total_buf, recv_t, c_buf, recv_c, e_send, recv_e, cnt_buf, recv_cnt,
    corr, recv_cz, corr_x, recv_cx,
    sem_cnt, rsem_cnt, sem_a, rsem_a, sem_s, rsem_s, sem_e, rsem_e, sem_t, rsem_t, sem_c, rsem_c,
    sem_cz, rsem_cz, sem_cx, rsem_cx,
):
    x, z, c, e = (lax.axis_index(name) for name in ("x", "z", "c", "e"))
    me = z * NC + c

    def zc_peers():
        for dz in Z_OFFSETS:
            for dc in (1, 0):
                if dz == 0 and dc == 0:
                    continue
                pz, pc = lax.rem(z + dz, NZ), lax.rem(c + dc, NC)
                yield pz * NC + pc, {"z": pz, "c": pc}

    def copy(src, dst, ssem, rsem, device):
        return pltpu.make_async_remote_copy(
            src_ref=src, dst_ref=dst, send_sem=ssem, recv_sem=rsem, device_id=device, device_id_type=MESH
        )

    recv_a[...] = jnp.zeros_like(recv_a)
    barrier = pltpu.get_barrier_semaphore()
    for _, device in zc_peers():
        pl.semaphore_signal(barrier, inc=1, device_id=device, device_id_type=MESH)
    for k in range(1, NX):
        pl.semaphore_signal(barrier, inc=1, device_id={"x": lax.rem(x + k, NX)}, device_id_type=MESH)
    for k in range(1, NE):
        pl.semaphore_signal(barrier, inc=1, device_id={"e": lax.rem(e + k, NE)}, device_id_type=MESH)

    contact = contact_ref[...].astype(F32)
    counts = jnp.sum(contact, axis=1, keepdims=True)
    cnt_buf[...] = jnp.zeros_like(cnt_buf)
    cnt_buf[0:4, :] = jnp.broadcast_to(counts, (4, LANES))
    pl.semaphore_wait(barrier, GROUP - 1 + NX - 1 + NE - 1)

    count_copies = []
    for k in range(1, NE):
        cp = copy(cnt_buf, recv_cnt.at[e], sem_cnt.at[k], rsem_cnt.at[e], {"e": lax.rem(e + k, NE)})
        cp.start()
        count_copies.append(cp)

    stiff, damp, grav = par_ref[0:1], par_ref[1:2], par_ref[2:3]
    cstiff, cdamp = par_ref[3:4], par_ref[4:5]
    lane = lax.broadcasted_iota(jnp.int32, (8, LANES), 1)
    row = lax.broadcasted_iota(jnp.int32, (8, LANES), 0)
    flip[...] = jnp.zeros_like(flip)
    flip[0:STATE, :] = init_ref[...]
    init_t[...] = jnp.transpose(flip[...])
    flip[...] = jnp.zeros_like(flip)
    flip[0:4, :] = contact
    contact8 = flip[0:8, :]
    for j in range(2):
        mine = row == jnp.where(lane < HALF, j, 2 + j)
        kk[j] = (stiff + exact_ta(contact8, jnp.where(mine, jnp.broadcast_to(cstiff, (8, LANES)), 0.0))) * TWO_PI
        dd[j] = (damp + exact_ta(contact8, jnp.where(mine, jnp.broadcast_to(cdamp, (8, LANES)), 0.0))) * (TWO_PI / H)
    flip[0:8, :] = jnp.zeros((8, ENV), F32)
    for j in range(2):
        flip[0:DOF, :] = torque_ref[j]
        flip[HALF : HALF + DOF, :] = torque_ref[2 + j]
        tau[j] = jnp.transpose(flip[...])
    hi, lo = split(block_ref[...] * (H * H / TWO_PI))
    nfine[0:LANES, 0:LANES] = hi
    nfine[0:LANES, LANES:] = lo
    nfine[LANES:, 0:LANES] = hi
    nfine[LANES:, LANES:] = lo

    sums = cnt_buf[...]
    for k in range(1, NE):
        p = lax.rem(e + k, NE)
        copy(cnt_buf, recv_cnt.at[p], sem_cnt.at[k], rsem_cnt.at[p], {"e": p}).wait_recv()
        sums = sums + recv_cnt[p]
    mean = sums * (1.0 / (ENV * NE))
    lane1 = lane[0:1]
    springs, frictions = [], []
    for j in range(2):
        m = jnp.where(lane1 < HALF, mean[j : j + 1], mean[2 + j : 3 + j])
        springs.append(stiff + grav + m * cstiff)
        frictions.append(damp + m * cdamp)

    def coarse(q, v, forced):
        for j in range(2):
            force = -(springs[j] * q + frictions[j] * v)
            if forced:
                force = force + tau[j]
            v = v + DT * exact(force, block_ref[...])
            q = q + DT * v
        return q, v

    eye = (
        lax.broadcasted_iota(jnp.int32, (LANES, LANES), 0) == lax.broadcasted_iota(jnp.int32, (LANES, LANES), 1)
    ).astype(F32)
    none = jnp.zeros((LANES, LANES), F32)
    mq, mv = coarse(jnp.concatenate([eye, none], axis=0), jnp.concatenate([none, eye], axis=0), False)
    mf = jnp.concatenate([mq, mv], axis=1)
    put_pair(mf_w, mf)
    map0 = exact_ta(pick_ref[0], exact(mf, pick_ref[0]))
    map1 = exact_ta(pick_ref[1], exact(mf, pick_ref[1]))
    a_buf[...] = exact(map0, map1)
    recv_a[me, 0:ROWS, :] = a_buf[0:ROWS, :]
    a_copies = []
    for p, device in zc_peers():
        cp = copy(
            a_buf.at[pl.ds(0, ROWS)], recv_a.at[me, pl.ds(0, ROWS)], sem_a.at[p], rsem_a.at[me], device
        )
        cp.start()
        a_copies.append(cp)
    put_pair(zf_w, exact(pick_ref[0], map1) + pick_ref[1])
    put_pair(ze_w, exact_tb(eye, pick_ref[0]) + exact_tb(map0, pick_ref[1]))

    fq, fv = coarse(jnp.zeros((ENV, LANES), F32), jnp.zeros((ENV, LANES), F32), True)
    free[:, 0:LANES] = fq
    free[:, LANES:] = fv
    jall[...] = jnp.zeros_like(jall)
    gee[...] = jnp.zeros_like(gee)
    ends[...] = jnp.zeros_like(ends)
    corr[...] = jnp.zeros_like(corr)
    for cp in count_copies:
        cp.wait_send()

    def fine():
        q_ref[...] = start[:, 0:LANES] * (1.0 / TWO_PI)
        v_ref[...] = start[:, LANES:] * (H / TWO_PI)
        coef = [grav * value for value in SINE]

        def horizon(j, unused):
            def substep(counter, unused2):
                for part in range(2):
                    rows = slice(part * (ENV // 2), (part + 1) * (ENV // 2))
                    q, v = q_ref[rows], v_ref[rows]
                    n = (q + MAGIC) - MAGIC
                    r = q - n
                    r2 = r * r
                    poly = coef[-1] * r2 + coef[-2]
                    for value in coef[-3::-1]:
                        poly = poly * r2 + value
                    force = tau[j, rows] - kk[j, rows] * q - dd[j, rows] * v - r * poly
                    hi, lo = split(force)
                    out = dot(jnp.concatenate([hi, lo], axis=1), nfine[...])
                    v = v + (out[:, 0:LANES] + out[:, LANES:])
                    v_ref[rows] = v
                    q_ref[rows] = q + v
                return unused2

            return lax.fori_loop(0, SUB, substep, unused, unroll=4)

        lax.fori_loop(0, 2, horizon, 0)
        free[:, 0:LANES] = q_ref[...] * TWO_PI
        free[:, LANES:] = v_ref[...] * (TWO_PI / H)

    def settle(slot):
        new = gee[...] + jall[...]
        change = new - ends[...]
        ends[...] = new
        square = change * change
        lanes2 = lax.broadcasted_iota(jnp.int32, (8, LANES), 1)
        first = (lanes2 < HALF).astype(F32)
        folded = square[:, 0:LANES] + square[:, LANES:]
        sum0 = exact_tb(first, folded)
        sum1 = exact_tb(1.0 - first, folded)
        corr[pl.ds(slot, 1), :] = jnp.sqrt(jnp.maximum(sum0, sum1))[0:1]

    def products():
        for i in range(4):
            acc = recv_a[4 * i]
            prod[4 * i + 0] = acc
            for j in range(1, 4):
                put_side(side_a, 4 * i + j, recv_a[4 * i + j])
                put_side(side_p, 4 * i + j, acc)
                acc = exact(acc, recv_a[4 * i + j])
                prod[4 * i + j] = acc
            put_side(side_b, i, acc)
        before = prod[3]
        for j in range(1, 4):
            put_side(side_pp, j, prod[j - 1])
        for i in range(1, 4):
            put_side(side_pp, 4 * i, before)
            for j in range(1, 4):
                put_side(side_pp, 4 * i + j, exact(before, prod[4 * i + j - 1]))
            before = exact(before, prod[4 * i + 3])
        c_buf[...] = before
        for k in range(1, NX):

            @pl.when(x + k < NX)
            def _():
                copy(c_buf, recv_c.at[x], sem_c.at[k], rsem_c.at[x], {"x": lax.rem(x + k, NX)}).start()

        for k in range(NX - 1):

            @pl.when(x > k)
            def _():
                copy(c_buf, recv_c.at[k], sem_c.at[k], rsem_c.at[k], {"x": k}).wait_recv()
                put_side(side_c, k, recv_c[k])

    def sweep(k, unused):
        @pl.when(k > 0)
        def _():
            fine()

        fresh = free[...] - gee[...]
        s_buf[...] = wide(fresh, zf_w)
        recv_s[k, me] = s_buf[pl.ds(me * BLOCK, BLOCK), :]
        s_copies = []
        for p, device in zc_peers():
            cp = copy(s_buf.at[pl.ds(p * BLOCK, BLOCK)], recv_s.at[k, me], sem_s.at[p], rsem_s.at[k, me], device)
            cp.start()
            s_copies.append(cp)

        settle(lax.max(k - 2, 0))
        jall[...] = fresh
        low = lax.broadcasted_iota(jnp.int32, (ENV, LANES), 1) < HALF
        for part in range(2):
            cols = slice(part * LANES, (part + 1) * LANES)
            jshift[:, cols] = jnp.where(low, 0.0, pltpu.roll(fresh[:, cols], HALF, 1))

        @pl.when(k == 0)
        def _():
            for p, device in zc_peers():
                copy(
                    a_buf.at[pl.ds(0, ROWS)], recv_a.at[p, pl.ds(0, ROWS)], sem_a.at[p], rsem_a.at[p], device
                ).wait_recv()
            products()

        for p, device in zc_peers():
            copy(s_buf.at[pl.ds(0, BLOCK)], recv_s.at[k, p], sem_s.at[p], rsem_s.at[k, p], device).wait_recv()

        inside = {}
        totals = []
        for i in range(4):
            acc = recv_s[k, 4 * i]
            for j in range(1, 4):
                inside[i, j] = acc
                acc = small(acc, side_a[4 * i + j]) + recv_s[k, 4 * i + j]
            totals.append(acc)
        entry = [None, totals[0]]
        for i in range(1, 4):
            entry.append(small(entry[i], side_b[i]) + totals[i])
        total_buf[...] = entry[4]
        for d in range(1, NX):

            @pl.when(x + d < NX)
            def _():
                copy(total_buf, recv_t.at[k, x], sem_t.at[d], rsem_t.at[k, x], {"x": lax.rem(x + d, NX)}).start()

        for i in range(4):
            if i > 0:
                ent[4 * i] = entry[i]
            for j in range(1, 4):
                value = inside[i, j]
                if i > 0:
                    value = small(entry[i], side_p[4 * i + j]) + value
                ent[4 * i + j] = value
        ent[0] = init_t[pl.ds(me * BLOCK, BLOCK), :]
        for d in range(NX - 1):

            @pl.when(x > d)
            def _():
                copy(total_buf, recv_t.at[k, d], sem_t.at[d], rsem_t.at[k, d], {"x": d}).wait_recv()
                ent[0] = small(ent[0], side_c[d]) + recv_t[k, d]

        first = ent[0]
        e_send[0] = first
        for d in range(1, GROUP):
            e_send[d] = small(first, side_pp[d]) + ent[d]
        recv_e[k, me] = e_send[me]
        e_copies = []
        for p, device in zc_peers():
            cp = copy(e_send.at[p], recv_e.at[k, me], sem_e.at[p], rsem_e.at[k, me], device)
            cp.start()
            e_copies.append(cp)
        for p, device in zc_peers():
            copy(e_send.at[p], recv_e.at[k, p], sem_e.at[p], rsem_e.at[k, p], device).wait_recv()

        arrived = recv_e[k].reshape(ENV, LANES)
        begin = wide(arrived, ze_w) + jshift[...]
        start[...] = begin
        gee[...] = wide(begin, mf_w)
        for cp in s_copies:
            cp.wait_send()
        for cp in e_copies:
            cp.wait_send()
        for d in range(1, NX):

            @pl.when(x + d < NX)
            def _():
                copy(total_buf, recv_t.at[k, x], sem_t.at[d], rsem_t.at[k, x], {"x": lax.rem(x + d, NX)}).wait_send()

        return unused

    lax.fori_loop(0, SWEEPS, sweep, 0)

    settle(ITERS - 1)
    cz_copies = []
    recv_cz[me] = corr[...]
    for p, device in zc_peers():
        cp = copy(corr, recv_cz.at[me], sem_cz.at[p], rsem_cz.at[me], device)
        cp.start()
        cz_copies.append(cp)
    for s in range(2):
        final_ref[s] = lax.dot_general(
            pick_ref[s], ends[...], (((0,), (1,)), ((), ())), precision=HIGHEST, preferred_element_type=F32
        )[0:STATE]
    for p, device in zc_peers():
        copy(corr, recv_cz.at[p], sem_cz.at[p], rsem_cz.at[p], device).wait_recv()
    corr_x[...] = jnp.max(recv_cz[...], axis=0)
    cx_copies = []
    for d in range(1, NX):
        cp = copy(corr_x, recv_cx.at[x], sem_cx.at[d], rsem_cx.at[x], {"x": lax.rem(x + d, NX)})
        cp.start()
        cx_copies.append(cp)
    best = corr_x[...]
    for d in range(1, NX):
        p = lax.rem(x + d, NX)
        copy(corr_x, recv_cx.at[p], sem_cx.at[d], rsem_cx.at[p], {"x": p}).wait_recv()
        best = jnp.maximum(best, recv_cx[p])
    corr_out_ref[...] = best[0:ITERS]
    for cp in a_copies + cz_copies + cx_copies:
        cp.wait_send()
    for k in range(1, NX):

        @pl.when(x + k < NX)
        def _():
            copy(c_buf, recv_c.at[x], sem_c.at[k], rsem_c.at[x], {"x": lax.rem(x + k, NX)}).wait_send()


def scratch():
    def v(*shape, dtype=F32):
        return pltpu.VMEM(shape, dtype)

    dma = pltpu.SemaphoreType.DMA
    return [
        v(LANES, ENV),
        v(2, ENV, LANES),
        v(2, ENV, LANES),
        v(2, ENV, LANES),
        v(ENV, LANES),
        v(ENV, LANES),
        v(ENV, LANES),
        v(2 * LANES, 2 * LANES, dtype=BF16),
        v(ENV, 2 * LANES),
        v(ENV, 2 * LANES),
        v(ENV, 2 * LANES),
        v(ENV, 2 * LANES),
        v(ENV, 2 * LANES),
        v(ENV, 2 * LANES),
        v(2, 2 * LANES, 2 * LANES, dtype=BF16),
        v(2, 2 * LANES, LANES, dtype=BF16),
        v(2, LANES, 2 * LANES, dtype=BF16),
        v(ENV, LANES),
        v(SWEEPS, GROUP, BLOCK, LANES),
        v(GROUP, LANES, LANES),
        v(LANES, LANES),
        v(GROUP, LANES, 2 * LANES, dtype=BF16),
        v(4, LANES, 2 * LANES, dtype=BF16),
        v(GROUP, LANES, 2 * LANES, dtype=BF16),
        v(GROUP, LANES, 2 * LANES, dtype=BF16),
        v(NX, LANES, 2 * LANES, dtype=BF16),
        v(GROUP, LANES, LANES),
        v(GROUP, BLOCK, LANES),
        v(BLOCK, LANES),
        v(SWEEPS, NX, BLOCK, LANES),
        v(LANES, LANES),
        v(NX, LANES, LANES),
        v(GROUP, BLOCK, LANES),
        v(SWEEPS, GROUP, BLOCK, LANES),
        v(8, LANES),
        v(NE, 8, LANES),
        v(8, ENV),
        v(GROUP, 8, ENV),
        v(8, ENV),
        v(NX, 8, ENV),
        dma((NE,)), dma((NE,)),
        dma((GROUP,)), dma((GROUP,)),
        dma((GROUP,)), dma((SWEEPS, GROUP)),
        dma((GROUP,)), dma((SWEEPS, GROUP)),
        dma((NX,)), dma((SWEEPS, NX)),
        dma((NX,)), dma((NX,)),
        dma((GROUP,)), dma((GROUP,)),
        dma((NX,)), dma((NX,)),
    ]


def shards(
    init_state, torque, contact, mass_inverse, stiffness, damping, gravity, contact_stiffness, contact_damping
):
    params = jnp.stack([stiffness, damping, gravity, contact_stiffness, contact_damping])
    params = jnp.pad(params, ((0, 3), (0, HALF - DOF)))
    params = jnp.concatenate([params, params], axis=1)
    blocks = jnp.pad(mass_inverse, ((0, 0), (0, HALF - DOF), (0, HALF - DOF)))
    zero = jnp.zeros((HALF, HALF), F32)
    block = jnp.concatenate(
        [jnp.concatenate([blocks[0], zero], axis=1), jnp.concatenate([zero, blocks[1]], axis=1)], axis=0
    )
    vmem = pl.BlockSpec(memory_space=pltpu.VMEM)
    return pl.pallas_call(
        body,
        out_shape=(
            jax.ShapeDtypeStruct((2, STATE, ENV), F32),
            jax.ShapeDtypeStruct((ITERS, ENV), F32),
        ),
        in_specs=[vmem] * 6,
        out_specs=(vmem, vmem),
        scratch_shapes=scratch(),
        compiler_params=pltpu.CompilerParams(collective_id=0, has_side_effects=True, vmem_limit_bytes=48 * 2**20),
        name="parareal",
    )(init_state, torque, contact, block, params, jnp.asarray(PICK))


def solution(mesh):
    torus = Mesh(mesh.devices.reshape(NX, NZ, NC, NE), ("x", "z", "c", "e"))
    return jax.shard_map(
        shards,
        mesh=torus,
        in_specs=(
            P(None, "e"),
            P(TM, None, "e"),
            P(TM, "e"),
            P(TM, None, None),
            P(),
            P(),
            P(),
            P(),
            P(),
        ),
        out_specs=(P(TM, None, "e"), P(None, "e")),
        check_vma=False,
    )
```

```python
import math

import jax
import jax.numpy as jnp
import numpy as np
from jax import lax
from jax.experimental import pallas as pl
from jax.experimental.pallas import tpu as pltpu
from jax.sharding import Mesh
from jax.sharding import PartitionSpec as P

DOF = 35
STATE = 70
SUB = 32
ITERS = 3
SWEEPS = ITERS + 1
NX, NZ, NC, NE = 4, 8, 2, 4
GROUP = NZ * NC
ENV = 256
BLOCK = ENV // GROUP
LANES = 128
HALF = 64
MROWS = 80
NROWS = 40
DT = 0.05
H = DT / SUB
TWO_PI = 2.0 * math.pi
MAGIC = 12582912.0
F32 = jnp.float32
BF16 = jnp.bfloat16
MESH = pl.DeviceIdType.MESH
HIGHEST = lax.Precision.HIGHEST
TM = ("x", "z", "c")
Z_OFFSETS = (4, 3, 5, 2, 6, 1, 7, 0)


def sine_coefficients(terms):
    x = np.cos(np.linspace(0, np.pi, 4001)) * 0.25 + 0.25
    x = x[x > 1e-4]
    basis = np.stack([x ** (2 * i + 1) for i in range(terms)], 1)
    target = np.sin(2 * np.pi * x)
    weight = np.ones_like(x)
    for _ in range(200):
        c = np.linalg.lstsq(basis * weight[:, None], target * weight, rcond=None)[0]
        weight = weight * (1e-12 + np.abs(basis @ c - target)) ** 0.1
        weight /= weight.mean()
    return [float(np.float32(v)) for v in c]


SINE = sine_coefficients(6)


def selectors():
    pick = np.zeros((2, 2 * LANES, LANES), np.float32)
    for s in range(2):
        for i in range(DOF):
            pick[s, HALF * s + i, i] = 1.0
            pick[s, LANES + HALF * s + i, DOF + i] = 1.0
    return pick


PICK = selectors()


def split(x):
    hi = x.astype(BF16)
    lo = (x - hi.astype(F32)).astype(BF16)
    return hi, lo


def split3(x):
    hi = x.astype(BF16)
    rest = x - hi.astype(F32)
    mid = rest.astype(BF16)
    return hi, mid, (rest - mid.astype(F32)).astype(BF16)


def dot(a, b):
    return jnp.dot(a, b, preferred_element_type=F32)


def exact(a, b):
    return jnp.dot(a, b, precision=HIGHEST, preferred_element_type=F32)


def exact_ta(a, b):
    return lax.dot_general(a, b, (((0,), (0,)), ((), ())), precision=HIGHEST, preferred_element_type=F32)


def exact_tb(a, b):
    return lax.dot_general(a, b, (((1,), (1,)), ((), ())), precision=HIGHEST, preferred_element_type=F32)


def wide(x, weights):
    hi, lo = split(x)
    return dot(hi, weights[0]) + dot(lo, weights[0]) + dot(hi, weights[1])


def pick_right(x, pick):
    hi, mid, lo = split3(x)
    return dot(hi, pick) + dot(mid, pick) + dot(lo, pick)


def pick_left(pick, x):
    hi, mid, lo = split3(x)
    return dot(pick, hi) + dot(pick, mid) + dot(pick, lo)


def put_pair(ref, value):
    hi, lo = split(value)
    ref[0] = hi
    ref[1] = lo


def put_side(ref, index, value):
    hi, lo = split(value)
    ref[index, 0:MROWS, 0:LANES] = hi
    ref[index, 0:MROWS, LANES:] = lo


def small(x, weights):
    rows = x.shape[0]
    hi, lo = split(x)
    out = dot(jnp.concatenate([hi, lo], axis=0), weights)
    both = out[:, 0:LANES] + out[:, LANES:]
    return both[0:rows] + both[rows:]


def body(
    init_in, torque_in, contact_in, minv_in, stiff_in, damp_in, grav_in, cstiff_in, cdamp_in, pick_in, turn_in,
    final_ref, corr_out_ref,
    init_ref, torque_ref, contact_ref, minv_ref, stiff_ref, damp_ref, grav_ref, cstiff_ref, cdamp_ref, pick_ref, turn_ref,
    in_sem, par_ref, block_ref, flip, tau, kk, dd, q_ref, v_ref, init_t, nfine, free, jall, start, gee, ends, jshift,
    mf_w, zf_w, ze_w, s_buf, recv_s, n_buf, recv_n, m_buf, recv_m, side_n, side_a, side_b, side_p, side_pp, side_c,
    prod, ent, total_buf, recv_t, c_buf, recv_c, e_send, recv_e, cnt_buf, recv_cnt,
    corr, recv_cz, corr_x, recv_cx,
    sem_cnt, rsem_cnt, sem_n, rsem_n, sem_m, rsem_m, sem_s, rsem_s, sem_e, rsem_e, sem_t, rsem_t, sem_c, rsem_c,
    sem_cz, rsem_cz, sem_cx, rsem_cx,
):
    x, z, c, e = (lax.axis_index(name) for name in ("x", "z", "c", "e"))
    me = z * NC + c

    def zc_peers():
        for dz in Z_OFFSETS:
            for dc in (1, 0):
                if dz == 0 and dc == 0:
                    continue
                pz, pc = lax.rem(z + dz, NZ), lax.rem(c + dc, NC)
                yield pz * NC + pc, {"z": pz, "c": pc}

    def copy(src, dst, ssem, rsem, device):
        return pltpu.make_async_remote_copy(
            src_ref=src, dst_ref=dst, send_sem=ssem, recv_sem=rsem, device_id=device, device_id_type=MESH
        )

    sources = (
        contact_in, minv_in, stiff_in, damp_in, grav_in, cstiff_in, cdamp_in, init_in, torque_in, pick_in, turn_in,
    )
    targets = (
        contact_ref, minv_ref, stiff_ref, damp_ref, grav_ref, cstiff_ref, cdamp_ref,
        init_ref, torque_ref, pick_ref, turn_ref,
    )
    loads = [pltpu.make_async_copy(a, b, in_sem.at[i]) for i, (a, b) in enumerate(zip(sources, targets))]
    for load in loads:
        load.start()
    barrier = pltpu.get_barrier_semaphore()
    for _, device in zc_peers():
        pl.semaphore_signal(barrier, inc=1, device_id=device, device_id_type=MESH)
    for k in range(1, NX):
        pl.semaphore_signal(barrier, inc=1, device_id={"x": lax.rem(x + k, NX)}, device_id_type=MESH)
    for k in range(1, NE):
        pl.semaphore_signal(barrier, inc=1, device_id={"e": lax.rem(e + k, NE)}, device_id_type=MESH)

    for side in (side_a, side_b, side_p, side_pp, side_c, side_n):
        side[...] = jnp.zeros_like(side)
    for load in loads:
        load.wait()
    contact = contact_ref[...].astype(F32)
    counts = jnp.sum(contact, axis=1, keepdims=True)
    cnt_buf[...] = jnp.zeros_like(cnt_buf)
    cnt_buf[0:4, :] = jnp.broadcast_to(counts, (4, LANES))
    lane = lax.broadcasted_iota(jnp.int32, (8, LANES), 1)
    row = lax.broadcasted_iota(jnp.int32, (8, LANES), 0)
    par_ref[...] = jnp.zeros_like(par_ref)
    for i, ref in enumerate((stiff_ref, damp_ref, grav_ref, cstiff_ref, cdamp_ref)):
        par_ref[i : i + 1, 0:DOF] = ref[...]
    par_one = par_ref[...]
    par_ref[...] = par_one + pltpu.roll(par_one, HALF, 1)
    flip[...] = jnp.zeros_like(flip)
    flip[0:DOF, 0:DOF] = minv_ref[:, 1, :]
    shifted = pltpu.roll(flip[0:NROWS, 0:LANES], HALF, 1)
    flip[0:DOF, 0:DOF] = minv_ref[:, 0, :]
    packed = flip[0:NROWS, 0:LANES] + shifted
    n_buf[...] = packed
    recv_n[me] = packed
    low40 = lax.broadcasted_iota(jnp.int32, (NROWS, LANES), 1) < HALF
    def clear(i, unused):
        block_ref[pl.ds(pl.multiple_of(i * HALF, HALF), HALF), :] = jnp.zeros((HALF, LANES), F32)
        return unused

    lax.fori_loop(0, 2, clear, 0)
    block_ref[0:NROWS, :] = jnp.where(low40, packed, 0.0)
    block_ref[HALF : HALF + NROWS, :] = jnp.where(low40, 0.0, packed)
    pl.semaphore_wait(barrier, GROUP - 1 + NX - 1 + NE - 1)

    count_copies = []
    for k in range(1, NE):
        cp = copy(cnt_buf, recv_cnt.at[e], sem_cnt.at[k], rsem_cnt.at[e], {"e": lax.rem(e + k, NE)})
        cp.start()
        count_copies.append(cp)
    n_copies = []
    for p, device in zc_peers():
        cp = copy(n_buf, recv_n.at[me], sem_n.at[p], rsem_n.at[me], device)
        cp.start()
        n_copies.append(cp)

    stiff, damp, grav = par_ref[0:1], par_ref[1:2], par_ref[2:3]
    cstiff, cdamp = par_ref[3:4], par_ref[4:5]
    flip[0:STATE, :] = init_ref[...]
    init_t[...] = jnp.transpose(flip[...])
    flip[...] = jnp.zeros_like(flip)
    flip[0:4, :] = contact
    contact8 = flip[0:8, :]
    for j in range(2):
        mine = row == jnp.where(lane < HALF, j, 2 + j)
        kk[j] = (stiff + exact_ta(contact8, jnp.where(mine, jnp.broadcast_to(cstiff, (8, LANES)), 0.0))) * TWO_PI
        dd[j] = (damp + exact_ta(contact8, jnp.where(mine, jnp.broadcast_to(cdamp, (8, LANES)), 0.0))) * (TWO_PI / H)
    flip[0:8, :] = jnp.zeros((8, ENV), F32)
    for j in range(2):
        flip[0:DOF, :] = torque_ref[:, j, :]
        flip[HALF : HALF + DOF, :] = torque_ref[:, 2 + j, :]
        tau[j] = jnp.transpose(flip[...])
    hi, lo = split(block_ref[...] * (H * H / TWO_PI))
    nfine[0:LANES, 0:LANES] = hi
    nfine[0:LANES, LANES:] = lo
    nfine[LANES:, 0:LANES] = hi
    nfine[LANES:, LANES:] = lo

    sums = cnt_buf[...]
    for k in range(1, NE):
        p = lax.rem(e + k, NE)
        copy(cnt_buf, recv_cnt.at[p], sem_cnt.at[k], rsem_cnt.at[p], {"e": p}).wait_recv()
        sums = sums + recv_cnt[p]
    mean = sums * (1.0 / (ENV * NE))
    m_buf[...] = mean
    recv_m[me] = mean
    m_copies = []
    for p, device in zc_peers():
        cp = copy(m_buf, recv_m.at[me], sem_m.at[p], rsem_m.at[me], device)
        cp.start()
        m_copies.append(cp)
    lane1 = lane[0:1]
    springs, frictions = [], []
    for j in range(2):
        m = jnp.where(lane1 < HALF, mean[j : j + 1], mean[2 + j : 3 + j])
        springs.append(stiff + grav + m * cstiff)
        frictions.append(damp + m * cdamp)

    def coarse(q, v, forced):
        for j in range(2):
            force = -(springs[j] * q + frictions[j] * v)
            if forced:
                force = force + tau[j]
            v = v + DT * exact(force, block_ref[...])
            q = q + DT * v
        return q, v

    eye = (
        lax.broadcasted_iota(jnp.int32, (LANES, LANES), 0) == lax.broadcasted_iota(jnp.int32, (LANES, LANES), 1)
    ).astype(F32)
    none = jnp.zeros((LANES, LANES), F32)
    mq, mv = coarse(jnp.concatenate([eye, none], axis=0), jnp.concatenate([none, eye], axis=0), False)
    mf = jnp.concatenate([mq, mv], axis=1)
    put_pair(mf_w, mf)
    map0 = pick_left(turn_ref[0], pick_right(mf, pick_ref[0]))
    map1 = pick_left(turn_ref[1], pick_right(mf, pick_ref[1]))
    put_pair(zf_w, pick_left(pick_ref[0], map1) + pick_ref[1].astype(F32))
    put_pair(ze_w, turn_ref[0].astype(F32) + pick_right(map0, turn_ref[1]))

    fq, fv = coarse(jnp.zeros((ENV, LANES), F32), jnp.zeros((ENV, LANES), F32), True)
    free[:, 0:LANES] = fq
    free[:, LANES:] = fv
    jall[...] = jnp.zeros_like(jall)
    gee[...] = jnp.zeros_like(gee)
    ends[...] = jnp.zeros_like(ends)
    corr[...] = jnp.zeros_like(corr)
    for cp in count_copies:
        cp.wait_send()

    def fine():
        q_ref[...] = start[:, 0:LANES] * (1.0 / TWO_PI)
        v_ref[...] = start[:, LANES:] * (H / TWO_PI)
        coef = [grav * value for value in SINE]

        def horizon(j, unused):
            def substep(counter, unused2):
                for part in range(2):
                    rows = slice(part * (ENV // 2), (part + 1) * (ENV // 2))
                    q, v = q_ref[rows], v_ref[rows]
                    n = (q + MAGIC) - MAGIC
                    r = q - n
                    r2 = r * r
                    poly = coef[-1] * r2 + coef[-2]
                    for value in coef[-3::-1]:
                        poly = poly * r2 + value
                    force = tau[j, rows] - kk[j, rows] * q - dd[j, rows] * v - r * poly
                    hi, lo = split(force)
                    out = dot(jnp.concatenate([hi, lo], axis=1), nfine[...])
                    v = v + (out[:, 0:LANES] + out[:, LANES:])
                    v_ref[rows] = v
                    q_ref[rows] = q + v
                return unused2

            return lax.fori_loop(0, SUB, substep, unused, unroll=4)

        lax.fori_loop(0, 2, horizon, 0)
        free[:, 0:LANES] = q_ref[...] * TWO_PI
        free[:, LANES:] = v_ref[...] * (TWO_PI / H)

    def settle(slot):
        new = gee[...] + jall[...]
        change = new - ends[...]
        ends[...] = new
        square = change * change
        lanes2 = lax.broadcasted_iota(jnp.int32, (8, LANES), 1)
        first = (lanes2 < HALF).astype(F32)
        folded = square[:, 0:LANES] + square[:, LANES:]
        sum0 = exact_tb(first, folded)
        sum1 = exact_tb(1.0 - first, folded)
        largest = jnp.sqrt(jnp.maximum(sum0, sum1))[0:1]
        corr[pl.ds(slot, 1), :] = largest[:, 0:LANES]
        corr[pl.ds(slot + 4, 1), :] = largest[:, LANES:]

    def maps(part, unused):
        rr = lax.broadcasted_iota(jnp.int32, (MROWS, LANES), 0)
        ll = lax.broadcasted_iota(jnp.int32, (MROWS, LANES), 1)
        base_q = ((rr == ll) & (ll < DOF)).astype(F32)
        base_v = ((rr == ll + DOF) & (ll < DOF)).astype(F32)
        keep = lane[0:1] < HALF
        one = [jnp.where(keep, par_ref[i : i + 1], 0.0) for i in range(5)]
        for u in range(8):
            p = part * 8 + u
            n_both = recv_n[p]
            means = recv_m[p]
            q, v = base_q, base_v
            for s in range(2):
                n_one = jnp.where(low40, pltpu.roll(n_both, HALF, 1) if s else n_both, 0.0)
                hi, lo = split(n_one)
                side_n[2 * u + s, 0:NROWS, 0:LANES] = hi
                side_n[2 * u + s, 0:NROWS, LANES:] = lo
                for j in range(2):
                    m = means[2 * s + j : 2 * s + j + 1]
                    spring = one[0] + one[2] + m * one[3]
                    friction = one[1] + m * one[4]
                    v = v - DT * small(spring * q + friction * v, side_n[2 * u + s])
                    q = q + DT * v
            full = q + pltpu.roll(v, DOF, 1)
            prod[p] = full
            put_side(side_a, p, full)
        return unused

    def products():
        lax.fori_loop(0, 2, maps, 0)
        for i in range(4):
            acc = prod[4 * i]
            for j in range(1, 4):
                put_side(side_p, 4 * i + j, acc)
                acc = small(acc, side_a[4 * i + j])
            put_side(side_b, i, acc)
            if i == 0:
                before = acc
        for j in range(1, 4):
            side_pp[j] = side_p[j]
        for i in range(1, 4):
            put_side(side_pp, 4 * i, before)
            for j in range(1, 4):
                put_side(side_pp, 4 * i + j, small(before, side_p[4 * i + j]))
            before = small(before, side_b[i])
        c_buf[...] = before
        for k in range(1, NX):

            @pl.when(x + k < NX)
            def _():
                copy(c_buf, recv_c.at[x], sem_c.at[k], rsem_c.at[x], {"x": lax.rem(x + k, NX)}).start()

    def sweep(k, unused):
        @pl.when(k > 0)
        def _():
            fine()

        fresh = free[...] - gee[...]
        s_buf[...] = wide(fresh, zf_w)
        recv_s[k, me] = s_buf[pl.ds(me * BLOCK, BLOCK), :]
        s_copies = []
        for p, device in zc_peers():
            cp = copy(s_buf.at[pl.ds(p * BLOCK, BLOCK)], recv_s.at[k, me], sem_s.at[p], rsem_s.at[k, me], device)
            cp.start()
            s_copies.append(cp)

        settle(lax.max(k - 2, 0))
        jall[...] = fresh
        low = lax.broadcasted_iota(jnp.int32, (ENV, LANES), 1) < HALF
        for part in range(2):
            cols = slice(part * LANES, (part + 1) * LANES)
            jshift[:, cols] = jnp.where(low, 0.0, pltpu.roll(fresh[:, cols], HALF, 1))

        @pl.when(k == 0)
        def _():
            for p, device in zc_peers():
                copy(n_buf, recv_n.at[p], sem_n.at[p], rsem_n.at[p], device).wait_recv()
            for p, device in zc_peers():
                copy(m_buf, recv_m.at[p], sem_m.at[p], rsem_m.at[p], device).wait_recv()
            products()

        for p, device in zc_peers():
            copy(s_buf.at[pl.ds(0, BLOCK)], recv_s.at[k, p], sem_s.at[p], rsem_s.at[k, p], device).wait_recv()

        inside = {}
        totals = []
        for i in range(4):
            acc = recv_s[k, 4 * i]
            for j in range(1, 4):
                inside[i, j] = acc
                acc = small(acc, side_a[4 * i + j]) + recv_s[k, 4 * i + j]
            totals.append(acc)
        entry = [None, totals[0]]
        for i in range(1, 4):
            entry.append(small(entry[i], side_b[i]) + totals[i])
        total_buf[...] = entry[4]
        for d in range(1, NX):

            @pl.when(x + d < NX)
            def _():
                copy(total_buf, recv_t.at[k, x], sem_t.at[d], rsem_t.at[k, x], {"x": lax.rem(x + d, NX)}).start()

        for i in range(4):
            if i > 0:
                ent[4 * i] = entry[i]
            for j in range(1, 4):
                value = inside[i, j]
                if i > 0:
                    value = small(entry[i], side_p[4 * i + j]) + value
                ent[4 * i + j] = value
        ent[0] = init_t[pl.ds(me * BLOCK, BLOCK), :]
        for d in range(NX - 1):

            @pl.when(x > d)
            def _():
                @pl.when(k == 0)
                def _():
                    copy(c_buf, recv_c.at[d], sem_c.at[d], rsem_c.at[d], {"x": d}).wait_recv()
                    put_side(side_c, d, recv_c[d])

                copy(total_buf, recv_t.at[k, d], sem_t.at[d], rsem_t.at[k, d], {"x": d}).wait_recv()
                ent[0] = small(ent[0], side_c[d]) + recv_t[k, d]

        first = ent[0]
        e_send[0] = first
        for d in range(1, GROUP):
            e_send[d] = small(first, side_pp[d]) + ent[d]
        recv_e[k, me] = e_send[me]
        e_copies = []
        for p, device in zc_peers():
            cp = copy(e_send.at[p], recv_e.at[k, me], sem_e.at[p], rsem_e.at[k, me], device)
            cp.start()
            e_copies.append(cp)
        for p, device in zc_peers():
            copy(e_send.at[p], recv_e.at[k, p], sem_e.at[p], rsem_e.at[k, p], device).wait_recv()

        arrived = recv_e[k].reshape(ENV, LANES)
        begin = wide(arrived, ze_w) + jshift[...]
        start[...] = begin
        gee[...] = wide(begin, mf_w)
        for cp in s_copies:
            cp.wait_send()
        for cp in e_copies:
            cp.wait_send()
        for d in range(1, NX):

            @pl.when(x + d < NX)
            def _():
                copy(total_buf, recv_t.at[k, x], sem_t.at[d], rsem_t.at[k, x], {"x": lax.rem(x + d, NX)}).wait_send()

        return unused

    lax.fori_loop(0, SWEEPS, sweep, 0)

    settle(ITERS - 1)
    cz_copies = []
    recv_cz[me] = corr[...]
    for p, device in zc_peers():
        cp = copy(corr, recv_cz.at[me], sem_cz.at[p], rsem_cz.at[me], device)
        cp.start()
        cz_copies.append(cp)
    for s in range(2):
        final_ref[:, s, :] = lax.dot_general(
            pick_ref[s].astype(F32), ends[...], (((0,), (1,)), ((), ())), precision=HIGHEST, preferred_element_type=F32
        )[0:STATE]
    for p, device in zc_peers():
        copy(corr, recv_cz.at[p], sem_cz.at[p], rsem_cz.at[p], device).wait_recv()
    corr_x[...] = jnp.max(recv_cz[...], axis=0)
    cx_copies = []
    for d in range(1, NX):
        cp = copy(corr_x, recv_cx.at[x], sem_cx.at[d], rsem_cx.at[x], {"x": lax.rem(x + d, NX)})
        cp.start()
        cx_copies.append(cp)
    best = corr_x[...]
    for d in range(1, NX):
        p = lax.rem(x + d, NX)
        copy(corr_x, recv_cx.at[p], sem_cx.at[d], rsem_cx.at[p], {"x": p}).wait_recv()
        best = jnp.maximum(best, recv_cx[p])
    corr_out_ref[:, 0:LANES] = best[0:ITERS]
    corr_out_ref[:, LANES:] = best[4 : 4 + ITERS]
    for cp in n_copies + m_copies + cz_copies + cx_copies:
        cp.wait_send()
    for k in range(1, NX):

        @pl.when(x + k < NX)
        def _():
            copy(c_buf, recv_c.at[x], sem_c.at[k], rsem_c.at[x], {"x": lax.rem(x + k, NX)}).wait_send()


def scratch():
    def v(*shape, dtype=F32):
        return pltpu.VMEM(shape, dtype)

    dma = pltpu.SemaphoreType.DMA
    return [
        v(STATE, ENV),
        v(DOF, 4, ENV),
        pltpu.VMEM((4, ENV), jnp.int32),
        v(DOF, 2, DOF),
        *[v(1, DOF) for _ in range(5)],
        v(2, 2 * LANES, LANES, dtype=BF16),
        v(2, LANES, 2 * LANES, dtype=BF16),
        dma((11,)),
        v(8, LANES),
        v(LANES, LANES),
        v(LANES, ENV),
        v(2, ENV, LANES),
        v(2, ENV, LANES),
        v(2, ENV, LANES),
        v(ENV, LANES),
        v(ENV, LANES),
        v(ENV, LANES),
        v(2 * LANES, 2 * LANES, dtype=BF16),
        v(ENV, 2 * LANES),
        v(ENV, 2 * LANES),
        v(ENV, 2 * LANES),
        v(ENV, 2 * LANES),
        v(ENV, 2 * LANES),
        v(ENV, 2 * LANES),
        v(2, 2 * LANES, 2 * LANES, dtype=BF16),
        v(2, 2 * LANES, LANES, dtype=BF16),
        v(2, LANES, 2 * LANES, dtype=BF16),
        v(ENV, LANES),
        v(SWEEPS, GROUP, BLOCK, LANES),
        v(NROWS, LANES),
        v(GROUP, NROWS, LANES),
        v(8, LANES),
        v(GROUP, 8, LANES),
        v(GROUP, LANES, 2 * LANES, dtype=BF16),
        v(GROUP, LANES, 2 * LANES, dtype=BF16),
        v(4, LANES, 2 * LANES, dtype=BF16),
        v(GROUP, LANES, 2 * LANES, dtype=BF16),
        v(GROUP, LANES, 2 * LANES, dtype=BF16),
        v(NX, LANES, 2 * LANES, dtype=BF16),
        v(GROUP, MROWS, LANES),
        v(GROUP, BLOCK, LANES),
        v(BLOCK, LANES),
        v(SWEEPS, NX, BLOCK, LANES),
        v(MROWS, LANES),
        v(NX, MROWS, LANES),
        v(GROUP, BLOCK, LANES),
        v(SWEEPS, GROUP, BLOCK, LANES),
        v(8, LANES),
        v(NE, 8, LANES),
        v(8, LANES),
        v(GROUP, 8, LANES),
        v(8, LANES),
        v(NX, 8, LANES),
        dma((NE,)), dma((NE,)),
        dma((GROUP,)), dma((GROUP,)),
        dma((GROUP,)), dma((GROUP,)),
        dma((GROUP,)), dma((SWEEPS, GROUP)),
        dma((GROUP,)), dma((SWEEPS, GROUP)),
        dma((NX,)), dma((SWEEPS, NX)),
        dma((NX,)), dma((NX,)),
        dma((GROUP,)), dma((GROUP,)),
        dma((NX,)), dma((NX,)),
    ]


def shards(
    init_state, torque, contact, mass_inverse, stiffness, damping, gravity, contact_stiffness, contact_damping
):
    params = [p.reshape(1, DOF) for p in (stiffness, damping, gravity, contact_stiffness, contact_damping)]
    vmem = pl.BlockSpec(memory_space=pltpu.VMEM)
    final, corrections = pl.pallas_call(
        body,
        out_shape=(
            jax.ShapeDtypeStruct((STATE, 2, ENV), F32),
            jax.ShapeDtypeStruct((ITERS, ENV), F32),
        ),
        in_specs=[pl.BlockSpec(memory_space=pltpu.HBM)] * 11,
        out_specs=(vmem, vmem),
        scratch_shapes=scratch(),
        compiler_params=pltpu.CompilerParams(collective_id=0, has_side_effects=True, vmem_limit_bytes=67043328),
        name="parareal",
    )(init_state, jnp.swapaxes(torque, 0, 1), contact, jnp.swapaxes(mass_inverse, 0, 1), *params, jnp.asarray(PICK, BF16), jnp.asarray(PICK.transpose(0, 2, 1), BF16))
    return jnp.swapaxes(final, 0, 1), corrections


def solution(mesh):
    torus = Mesh(mesh.devices.reshape(NX, NZ, NC, NE), ("x", "z", "c", "e"))
    return jax.shard_map(
        shards,
        mesh=torus,
        in_specs=(
            P(None, "e"),
            P(TM, None, "e"),
            P(TM, "e"),
            P(TM, None, None),
            P(),
            P(),
            P(),
            P(),
            P(),
        ),
        out_specs=(P(TM, None, "e"), P(None, "e")),
        check_vma=False,
    )
```

```python
import math

import jax
import jax.numpy as jnp
import numpy as np
from jax import lax
from jax.experimental import pallas as pl
from jax.experimental.pallas import tpu as pltpu
from jax.sharding import Mesh
from jax.sharding import PartitionSpec as P

DOF = 35
STATE = 70
SUB = 32
ITERS = 3
SWEEPS = ITERS + 1
NX, NZ, NC, NE = 4, 8, 2, 4
GROUP = NZ * NC
ENV = 256
BLOCK = ENV // GROUP
LANES = 128
HALF = 64
MROWS = 80
NROWS = 40
DT = 0.05
H = DT / SUB
TWO_PI = 2.0 * math.pi
F32 = jnp.float32
BF16 = jnp.bfloat16
MESH = pl.DeviceIdType.MESH
HIGHEST = lax.Precision.HIGHEST
TM = ("x", "z", "c")
Z_OFFSETS = (4, 3, 5, 2, 6, 1, 7, 0)
NEAR_FIRST = ((0, 1, 7, 2), (6, 3, 5, 4))
NEAR_CHIPS = (1, 7, 2, 6, 3, 5, 4)


def sine_coefficients(terms):
    x = np.cos(np.linspace(0, np.pi, 4001)) * 0.25 + 0.25
    x = x[x > 1e-4]
    basis = np.stack([x ** (2 * i + 1) for i in range(terms)], 1)
    target = np.sin(2 * np.pi * x)
    weight = np.ones_like(x)
    for _ in range(200):
        c = np.linalg.lstsq(basis * weight[:, None], target * weight, rcond=None)[0]
        weight = weight * (1e-12 + np.abs(basis @ c - target)) ** 0.1
        weight /= weight.mean()
    return [float(np.float32(v)) for v in c]


SINE = sine_coefficients(6)


def selectors():
    pick = np.zeros((2, 2 * LANES, LANES), np.float32)
    for s in range(2):
        for i in range(DOF):
            pick[s, HALF * s + i, i] = 1.0
            pick[s, LANES + HALF * s + i, DOF + i] = 1.0
    return pick


PICK = selectors()


def split(x):
    hi = x.astype(BF16)
    lo = (x - hi.astype(F32)).astype(BF16)
    return hi, lo


def split3(x):
    hi = x.astype(BF16)
    rest = x - hi.astype(F32)
    mid = rest.astype(BF16)
    return hi, mid, (rest - mid.astype(F32)).astype(BF16)


def dot(a, b):
    return jnp.dot(a, b, preferred_element_type=F32)


def exact(a, b):
    return jnp.dot(a, b, precision=HIGHEST, preferred_element_type=F32)


def exact_ta(a, b):
    return lax.dot_general(a, b, (((0,), (0,)), ((), ())), precision=HIGHEST, preferred_element_type=F32)


def exact_tb(a, b):
    return lax.dot_general(a, b, (((1,), (1,)), ((), ())), precision=HIGHEST, preferred_element_type=F32)


def wide(x, weights):
    hi, lo = split(x)
    return dot(hi, weights[0]) + dot(lo, weights[0]) + dot(hi, weights[1])


def pick_right(x, pick):
    hi, mid, lo = split3(x)
    return dot(hi, pick) + dot(mid, pick) + dot(lo, pick)


def pick_left(pick, x):
    hi, mid, lo = split3(x)
    return dot(pick, hi) + dot(pick, mid) + dot(pick, lo)


def put_pair(ref, value):
    hi, lo = split(value)
    ref[0] = hi
    ref[1] = lo


def put_side(ref, index, value):
    hi, lo = split(value)
    ref[index, 0:MROWS, 0:LANES] = hi
    ref[index, 0:MROWS, LANES:] = lo


def small(x, weights):
    rows = x.shape[0]
    hi, lo = split(x)
    out = dot(jnp.concatenate([hi, lo], axis=0), weights)
    both = out[:, 0:LANES] + out[:, LANES:]
    return both[0:rows] + both[rows:]


def body(
    init_in, torque_in, contact_in, minv_in, stiff_in, damp_in, grav_in, cstiff_in, cdamp_in, pick_in, turn_in,
    final_ref, corr_out_ref,
    init_ref, torque_ref, contact_ref, minv_ref, stiff_ref, damp_ref, grav_ref, cstiff_ref, cdamp_ref, pick_ref, turn_ref,
    in_sem, par_ref, block_ref, flip, tau, kk, dd, q_ref, v_ref, init_t, nfine, free, jall, start, gee, ends, jshift,
    mf_w, zf_w, ze_w, s_buf, recv_s, n_buf, recv_n, m_buf, recv_m, side_n, side_a, side_b, side_p, side_pp, side_c,
    prod, ent, total_buf, recv_t, c_buf, recv_c, e_send, recv_e, cnt_buf, recv_cnt,
    corr, recv_cz, corr_x, recv_cx,
    sem_cnt, rsem_cnt, sem_n, rsem_n, sem_m, rsem_m, sem_p, rsem_p, sem_s, rsem_s, sem_e, rsem_e, sem_t, rsem_t, sem_c, rsem_c,
    sem_cz, rsem_cz, sem_cx, rsem_cx,
):
    x, z, c, e = (lax.axis_index(name) for name in ("x", "z", "c", "e"))
    me = z * NC + c

    def zc_peers():
        for dz in Z_OFFSETS:
            for dc in (1, 0):
                if dz == 0 and dc == 0:
                    continue
                pz, pc = lax.rem(z + dz, NZ), lax.rem(c + dc, NC)
                yield pz * NC + pc, {"z": pz, "c": pc}

    def chips(offsets):
        for dz in offsets:
            pz = lax.rem(z + dz, NZ)
            yield pz, {"z": pz}

    def copy(src, dst, ssem, rsem, device):
        return pltpu.make_async_remote_copy(
            src_ref=src, dst_ref=dst, send_sem=ssem, recv_sem=rsem, device_id=device, device_id_type=MESH
        )

    sources = (
        contact_in, minv_in, stiff_in, damp_in, grav_in, cstiff_in, cdamp_in, init_in, torque_in, pick_in, turn_in,
    )
    targets = (
        contact_ref, minv_ref, stiff_ref, damp_ref, grav_ref, cstiff_ref, cdamp_ref,
        init_ref, torque_ref, pick_ref, turn_ref,
    )
    loads = [pltpu.make_async_copy(a, b, in_sem.at[i]) for i, (a, b) in enumerate(zip(sources, targets))]
    for load in loads:
        load.start()
    barrier = pltpu.get_barrier_semaphore()
    for _, device in zc_peers():
        pl.semaphore_signal(barrier, inc=1, device_id=device, device_id_type=MESH)
    for k in range(1, NX):
        pl.semaphore_signal(barrier, inc=1, device_id={"x": lax.rem(x + k, NX)}, device_id_type=MESH)
    for k in range(1, NE):
        pl.semaphore_signal(barrier, inc=1, device_id={"e": lax.rem(e + k, NE)}, device_id_type=MESH)

    for side in (side_a, side_b, side_p, side_pp, side_c, side_n):
        side[...] = jnp.zeros_like(side)
    for load in loads:
        load.wait()
    contact = contact_ref[...].astype(F32)
    counts = jnp.sum(contact, axis=1, keepdims=True)
    cnt_buf[...] = jnp.zeros_like(cnt_buf)
    cnt_buf[0:4, :] = jnp.broadcast_to(counts, (4, LANES))
    lane = lax.broadcasted_iota(jnp.int32, (8, LANES), 1)
    row = lax.broadcasted_iota(jnp.int32, (8, LANES), 0)
    par_ref[...] = jnp.zeros_like(par_ref)
    for i, ref in enumerate((stiff_ref, damp_ref, grav_ref, cstiff_ref, cdamp_ref)):
        par_ref[i : i + 1, 0:DOF] = ref[...]
    par_one = par_ref[...]
    par_ref[...] = par_one + pltpu.roll(par_one, HALF, 1)
    flip[...] = jnp.zeros_like(flip)
    flip[0:DOF, 0:DOF] = minv_ref[:, 1, :]
    shifted = pltpu.roll(flip[0:NROWS, 0:LANES], HALF, 1)
    flip[0:DOF, 0:DOF] = minv_ref[:, 0, :]
    packed = flip[0:NROWS, 0:LANES] + shifted
    n_buf[...] = packed
    recv_n[z] = packed
    low40 = lax.broadcasted_iota(jnp.int32, (NROWS, LANES), 1) < HALF
    def clear(i, unused):
        block_ref[pl.ds(pl.multiple_of(i * HALF, HALF), HALF), :] = jnp.zeros((HALF, LANES), F32)
        return unused

    lax.fori_loop(0, 2, clear, 0)
    block_ref[0:NROWS, :] = jnp.where(low40, packed, 0.0)
    block_ref[HALF : HALF + NROWS, :] = jnp.where(low40, 0.0, packed)
    pl.semaphore_wait(barrier, GROUP - 1 + NX - 1 + NE - 1)

    count_copies = []
    for k in range(1, NE):
        cp = copy(cnt_buf, recv_cnt.at[e], sem_cnt.at[k], rsem_cnt.at[e], {"e": lax.rem(e + k, NE)})
        cp.start()
        count_copies.append(cp)
    n_copies = []
    for p, device in chips(NEAR_CHIPS):
        cp = copy(n_buf, recv_n.at[z], sem_n.at[p], rsem_n.at[z], device)
        cp.start()
        n_copies.append(cp)

    stiff, damp, grav = par_ref[0:1], par_ref[1:2], par_ref[2:3]
    cstiff, cdamp = par_ref[3:4], par_ref[4:5]
    flip[0:STATE, :] = init_ref[...]
    init_t[...] = jnp.transpose(flip[...])
    flip[...] = jnp.zeros_like(flip)
    flip[0:4, :] = contact
    contact8 = flip[0:8, :]
    for j in range(2):
        mine = row == jnp.where(lane < HALF, j, 2 + j)
        kk[j] = (stiff + exact_ta(contact8, jnp.where(mine, jnp.broadcast_to(cstiff, (8, LANES)), 0.0))) * TWO_PI
        dd[j] = (damp + exact_ta(contact8, jnp.where(mine, jnp.broadcast_to(cdamp, (8, LANES)), 0.0))) * (TWO_PI / H)
    flip[0:8, :] = jnp.zeros((8, ENV), F32)
    for j in range(2):
        flip[0:DOF, :] = torque_ref[:, j, :]
        flip[HALF : HALF + DOF, :] = torque_ref[:, 2 + j, :]
        tau[j] = jnp.transpose(flip[...])
    hi, lo = split(block_ref[...] * (H * H / TWO_PI))
    nfine[0:LANES, 0:LANES] = hi
    nfine[0:LANES, LANES:] = lo
    nfine[LANES:, 0:LANES] = hi
    nfine[LANES:, LANES:] = lo

    sums = cnt_buf[...]
    for k in range(1, NE):
        p = lax.rem(e + k, NE)
        copy(cnt_buf, recv_cnt.at[p], sem_cnt.at[k], rsem_cnt.at[p], {"e": p}).wait_recv()
        sums = sums + recv_cnt[p]
    mean = sums * (1.0 / (ENV * NE))
    m_buf[...] = mean
    recv_m[z] = mean
    m_copies = []
    for p, device in chips(NEAR_CHIPS):
        cp = copy(m_buf, recv_m.at[z], sem_m.at[p], rsem_m.at[z], device)
        cp.start()
        m_copies.append(cp)
    lane1 = lane[0:1]
    springs, frictions = [], []
    for j in range(2):
        m = jnp.where(lane1 < HALF, mean[j : j + 1], mean[2 + j : 3 + j])
        springs.append(stiff + grav + m * cstiff)
        frictions.append(damp + m * cdamp)

    def coarse(q, v, forced):
        for j in range(2):
            force = -(springs[j] * q + frictions[j] * v)
            if forced:
                force = force + tau[j]
            v = v + DT * exact(force, block_ref[...])
            q = q + DT * v
        return q, v

    eye = (
        lax.broadcasted_iota(jnp.int32, (LANES, LANES), 0) == lax.broadcasted_iota(jnp.int32, (LANES, LANES), 1)
    ).astype(F32)
    none = jnp.zeros((LANES, LANES), F32)
    mq, mv = coarse(jnp.concatenate([eye, none], axis=0), jnp.concatenate([none, eye], axis=0), False)
    mf = jnp.concatenate([mq, mv], axis=1)
    put_pair(mf_w, mf)
    map0 = pick_left(turn_ref[0], pick_right(mf, pick_ref[0]))
    map1 = pick_left(turn_ref[1], pick_right(mf, pick_ref[1]))
    hi, lo = split(pick_left(pick_ref[0], map1) + pick_ref[1].astype(F32))
    zf_w[:, 0:LANES] = hi
    zf_w[:, LANES:] = lo
    place = turn_ref[0].astype(F32) + pick_right(map0, turn_ref[1])
    for part, value in enumerate((place, wide(place, mf_w))):
        hi, lo = split(value)
        cols = slice(2 * LANES * part, 2 * LANES * (part + 1))
        ze_w[0:LANES, cols] = hi
        ze_w[LANES : 2 * LANES, cols] = hi
        ze_w[2 * LANES :, cols] = lo

    fq, fv = coarse(jnp.zeros((ENV, LANES), F32), jnp.zeros((ENV, LANES), F32), True)
    free[:, 0:LANES] = fq
    free[:, LANES:] = fv
    jall[...] = jnp.zeros_like(jall)
    gee[...] = jnp.zeros_like(gee)
    ends[...] = jnp.zeros_like(ends)
    corr[...] = jnp.zeros_like(corr)
    for cp in count_copies:
        cp.wait_send()

    def fine():
        q_ref[...] = start[:, 0:LANES] * (1.0 / TWO_PI)
        v_ref[...] = start[:, LANES:] * (H / TWO_PI)
        coef = [grav * value for value in SINE]

        def horizon(j, unused):
            def substep(counter, unused2):
                q, v = q_ref[...], v_ref[...]
                r = q - jnp.round(q)
                r2 = r * r
                r4 = r2 * r2
                low, mid, high = (coef[i + 1] * r2 + coef[i] for i in (0, 2, 4))
                poly = (high * r4 + mid) * r4 + low
                force = tau[j] - kk[j] * q - dd[j] * v - r * poly
                hi, lo = split(force)
                out = dot(jnp.concatenate([hi, lo], axis=1), nfine[...])
                v = v + (out[:, 0:LANES] + out[:, LANES:])
                v_ref[...] = v
                q_ref[...] = q + v
                return unused2

            return lax.fori_loop(0, SUB, substep, unused, unroll=16)

        lax.fori_loop(0, 2, horizon, 0)
        free[:, 0:LANES] = q_ref[...] * TWO_PI
        free[:, LANES:] = v_ref[...] * (TWO_PI / H)

    def settle(slot):
        new = gee[...] + jall[...]
        change = new - ends[...]
        ends[...] = new
        square = change * change
        lanes2 = lax.broadcasted_iota(jnp.int32, (8, LANES), 1)
        first = (lanes2 < HALF).astype(F32)
        folded = square[:, 0:LANES] + square[:, LANES:]
        sum0 = exact_tb(first, folded)
        sum1 = exact_tb(1.0 - first, folded)
        largest = jnp.sqrt(jnp.maximum(sum0, sum1))[0:1]
        corr[pl.ds(slot, 1), :] = largest[:, 0:LANES]
        corr[pl.ds(slot + 4, 1), :] = largest[:, LANES:]

    def maps(offsets):
        rr = lax.broadcasted_iota(jnp.int32, (MROWS, LANES), 0)
        ll = lax.broadcasted_iota(jnp.int32, (MROWS, LANES), 1)
        base_q = ((rr == ll) & (ll < DOF)).astype(F32)
        base_v = ((rr == ll + DOF) & (ll < DOF)).astype(F32)
        keep = lane[0:1] < HALF
        one = [jnp.where(keep, par_ref[i : i + 1], 0.0) for i in range(5)]
        for p, device in chips([dz for dz in offsets if dz]):
            copy(n_buf, recv_n.at[p], sem_n.at[p], rsem_n.at[p], device).wait_recv()
            copy(m_buf, recv_m.at[p], sem_m.at[p], rsem_m.at[p], device).wait_recv()
        for u, (p, _) in enumerate(chips(offsets)):
            n_both = recv_n[p]
            means = recv_m[p]
            q, v = base_q, base_v
            for s in range(2):
                n_one = jnp.where(low40, pltpu.roll(n_both, HALF, 1) if s else n_both, 0.0)
                hi, lo = split(n_one)
                side_n[2 * u + s, 0:NROWS, 0:LANES] = hi
                side_n[2 * u + s, 0:NROWS, LANES:] = lo
                for j in range(2):
                    m = means[2 * s + j : 2 * s + j + 1]
                    spring = one[0] + one[2] + m * one[3]
                    friction = one[1] + m * one[4]
                    v = v - DT * small(spring * q + friction * v, side_n[2 * u + s])
                    q = q + DT * v
            prod[p * NC + c] = q + pltpu.roll(v, DOF, 1)
        for p, _ in chips(offsets):
            swap(p * NC + c, p).start()

    def swap(slot, p):
        return copy(prod.at[slot], prod.at[slot], sem_p.at[p], rsem_p.at[p], {"c": 1 - c})

    def products():
        for offsets in NEAR_FIRST:
            maps(offsets)
        for p in range(NZ):
            put_side(side_a, p * NC + c, prod[p * NC + c])
        for p in range(NZ):
            swap(p * NC + 1 - c, p).wait_recv()
            put_side(side_a, p * NC + 1 - c, prod[p * NC + 1 - c])
        for i in range(4):
            acc = prod[4 * i]
            for j in range(1, 4):
                put_side(side_p, 4 * i + j, acc)
                acc = small(acc, side_a[4 * i + j])
            put_side(side_b, i, acc)
            if i == 0:
                before = acc
        for j in range(1, 4):
            side_pp[j] = side_p[j]
        for i in range(1, 4):
            put_side(side_pp, 4 * i, before)
            for j in range(1, 4):
                put_side(side_pp, 4 * i + j, small(before, side_p[4 * i + j]))
            before = small(before, side_b[i])
        c_buf[...] = before
        for k in range(1, NX):

            @pl.when(x + k < NX)
            def _():
                copy(c_buf, recv_c.at[x], sem_c.at[k], rsem_c.at[x], {"x": lax.rem(x + k, NX)}).start()

    def sweep(k, unused):
        @pl.when(k > 0)
        def _():
            fine()

        fresh = free[...] - gee[...]
        hi, lo = split(fresh)
        shifts = dot(hi, zf_w[...]) + dot(lo, zf_w[...])
        s_buf[...] = shifts[:, 0:LANES] + shifts[:, LANES:]
        recv_s[k, me] = s_buf[pl.ds(me * BLOCK, BLOCK), :]
        s_copies = []
        for p, device in zc_peers():
            cp = copy(s_buf.at[pl.ds(p * BLOCK, BLOCK)], recv_s.at[k, me], sem_s.at[p], rsem_s.at[k, me], device)
            cp.start()
            s_copies.append(cp)

        settle(lax.max(k - 2, 0))
        jall[...] = fresh
        low = lax.broadcasted_iota(jnp.int32, (ENV, LANES), 1) < HALF
        for part in range(2):
            cols = slice(part * LANES, (part + 1) * LANES)
            jshift[:, cols] = jnp.where(low, 0.0, pltpu.roll(fresh[:, cols], HALF, 1))
        jshift[:, 2 * LANES :] = wide(jshift[:, 0 : 2 * LANES], mf_w)

        @pl.when(k == 0)
        def _():
            products()

        for p, device in zc_peers():
            copy(s_buf.at[pl.ds(0, BLOCK)], recv_s.at[k, p], sem_s.at[p], rsem_s.at[k, p], device).wait_recv()

        inside = {}
        totals = []
        for i in range(4):
            acc = recv_s[k, 4 * i]
            for j in range(1, 4):
                inside[i, j] = acc
                acc = small(acc, side_a[4 * i + j]) + recv_s[k, 4 * i + j]
            totals.append(acc)
        entry = [None, totals[0]]
        for i in range(1, 4):
            entry.append(small(entry[i], side_b[i]) + totals[i])
        total_buf[...] = entry[4]
        for d in range(1, NX):

            @pl.when(x + d < NX)
            def _():
                copy(total_buf, recv_t.at[k, x], sem_t.at[d], rsem_t.at[k, x], {"x": lax.rem(x + d, NX)}).start()

        for i in range(4):
            if i > 0:
                ent[4 * i] = entry[i]
            for j in range(1, 4):
                value = inside[i, j]
                if i > 0:
                    value = small(entry[i], side_p[4 * i + j]) + value
                ent[4 * i + j] = value
        ent[0] = init_t[pl.ds(me * BLOCK, BLOCK), :]
        for d in range(NX - 1):

            @pl.when(x > d)
            def _():
                @pl.when(k == 0)
                def _():
                    copy(c_buf, recv_c.at[d], sem_c.at[d], rsem_c.at[d], {"x": d}).wait_recv()
                    put_side(side_c, d, recv_c[d])

                copy(total_buf, recv_t.at[k, d], sem_t.at[d], rsem_t.at[k, d], {"x": d}).wait_recv()
                ent[0] = small(ent[0], side_c[d]) + recv_t[k, d]

        first = ent[0]
        e_send[0] = first
        for d in range(1, GROUP):
            e_send[d] = small(first, side_pp[d]) + ent[d]
        recv_e[k, me] = e_send[me]
        e_copies = []
        for p, device in zc_peers():
            cp = copy(e_send.at[p], recv_e.at[k, me], sem_e.at[p], rsem_e.at[k, me], device)
            cp.start()
            e_copies.append(cp)
        for p, device in zc_peers():
            copy(e_send.at[p], recv_e.at[k, p], sem_e.at[p], rsem_e.at[k, p], device).wait_recv()

        arrived = recv_e[k].reshape(ENV, LANES)
        hi, lo = split(arrived)
        both = dot(jnp.concatenate([hi, lo], axis=1), ze_w[0 : 2 * LANES, :]) + dot(hi, ze_w[2 * LANES :, :])
        start[...] = both[:, 0 : 2 * LANES] + jshift[:, 0 : 2 * LANES]
        gee[...] = both[:, 2 * LANES :] + jshift[:, 2 * LANES :]
        for cp in s_copies:
            cp.wait_send()
        for cp in e_copies:
            cp.wait_send()
        for d in range(1, NX):

            @pl.when(x + d < NX)
            def _():
                copy(total_buf, recv_t.at[k, x], sem_t.at[d], rsem_t.at[k, x], {"x": lax.rem(x + d, NX)}).wait_send()

        return unused

    lax.fori_loop(0, SWEEPS, sweep, 0)

    settle(ITERS - 1)
    cz_copies = []
    recv_cz[me] = corr[...]
    for p, device in zc_peers():
        cp = copy(corr, recv_cz.at[me], sem_cz.at[p], rsem_cz.at[me], device)
        cp.start()
        cz_copies.append(cp)
    for s in range(2):
        final_ref[:, s, :] = lax.dot_general(
            pick_ref[s].astype(F32), ends[...], (((0,), (1,)), ((), ())), precision=HIGHEST, preferred_element_type=F32
        )[0:STATE]
    for p, device in zc_peers():
        copy(corr, recv_cz.at[p], sem_cz.at[p], rsem_cz.at[p], device).wait_recv()
    corr_x[...] = jnp.max(recv_cz[...], axis=0)
    cx_copies = []
    for d in range(1, NX):
        cp = copy(corr_x, recv_cx.at[x], sem_cx.at[d], rsem_cx.at[x], {"x": lax.rem(x + d, NX)})
        cp.start()
        cx_copies.append(cp)
    best = corr_x[...]
    for d in range(1, NX):
        p = lax.rem(x + d, NX)
        copy(corr_x, recv_cx.at[p], sem_cx.at[d], rsem_cx.at[p], {"x": p}).wait_recv()
        best = jnp.maximum(best, recv_cx[p])
    corr_out_ref[:, 0:LANES] = best[0:ITERS]
    corr_out_ref[:, LANES:] = best[4 : 4 + ITERS]
    for p in range(NZ):
        swap(p * NC + c, p).wait_send()
    for cp in n_copies + m_copies + cz_copies + cx_copies:
        cp.wait_send()
    for k in range(1, NX):

        @pl.when(x + k < NX)
        def _():
            copy(c_buf, recv_c.at[x], sem_c.at[k], rsem_c.at[x], {"x": lax.rem(x + k, NX)}).wait_send()


def scratch():
    def v(*shape, dtype=F32):
        return pltpu.VMEM(shape, dtype)

    dma = pltpu.SemaphoreType.DMA
    return [
        v(STATE, ENV),
        v(DOF, 4, ENV),
        pltpu.VMEM((4, ENV), jnp.int32),
        v(DOF, 2, DOF),
        *[v(1, DOF) for _ in range(5)],
        v(2, 2 * LANES, LANES, dtype=BF16),
        v(2, LANES, 2 * LANES, dtype=BF16),
        dma((11,)),
        v(8, LANES),
        v(LANES, LANES),
        v(LANES, ENV),
        v(2, ENV, LANES),
        v(2, ENV, LANES),
        v(2, ENV, LANES),
        v(ENV, LANES),
        v(ENV, LANES),
        v(ENV, LANES),
        v(2 * LANES, 2 * LANES, dtype=BF16),
        v(ENV, 2 * LANES),
        v(ENV, 2 * LANES),
        v(ENV, 2 * LANES),
        v(ENV, 2 * LANES),
        v(ENV, 2 * LANES),
        v(ENV, 4 * LANES),
        v(2, 2 * LANES, 2 * LANES, dtype=BF16),
        v(2 * LANES, 2 * LANES, dtype=BF16),
        v(3 * LANES, 4 * LANES, dtype=BF16),
        v(ENV, LANES),
        v(SWEEPS, GROUP, BLOCK, LANES),
        v(NROWS, LANES),
        v(NZ, NROWS, LANES),
        v(8, LANES),
        v(NZ, 8, LANES),
        v(8, LANES, 2 * LANES, dtype=BF16),
        v(GROUP, LANES, 2 * LANES, dtype=BF16),
        v(4, LANES, 2 * LANES, dtype=BF16),
        v(GROUP, LANES, 2 * LANES, dtype=BF16),
        v(GROUP, LANES, 2 * LANES, dtype=BF16),
        v(NX, LANES, 2 * LANES, dtype=BF16),
        v(GROUP, MROWS, LANES),
        v(GROUP, BLOCK, LANES),
        v(BLOCK, LANES),
        v(SWEEPS, NX, BLOCK, LANES),
        v(MROWS, LANES),
        v(NX, MROWS, LANES),
        v(GROUP, BLOCK, LANES),
        v(SWEEPS, GROUP, BLOCK, LANES),
        v(8, LANES),
        v(NE, 8, LANES),
        v(8, LANES),
        v(GROUP, 8, LANES),
        v(8, LANES),
        v(NX, 8, LANES),
        dma((NE,)), dma((NE,)),
        dma((NZ,)), dma((NZ,)),
        dma((NZ,)), dma((NZ,)),
        dma((NZ,)), dma((NZ,)),
        dma((GROUP,)), dma((SWEEPS, GROUP)),
        dma((GROUP,)), dma((SWEEPS, GROUP)),
        dma((NX,)), dma((SWEEPS, NX)),
        dma((NX,)), dma((NX,)),
        dma((GROUP,)), dma((GROUP,)),
        dma((NX,)), dma((NX,)),
    ]


def shards(
    init_state, torque, contact, mass_inverse, stiffness, damping, gravity, contact_stiffness, contact_damping
):
    params = [p.reshape(1, DOF) for p in (stiffness, damping, gravity, contact_stiffness, contact_damping)]
    vmem = pl.BlockSpec(memory_space=pltpu.VMEM)
    final, corrections = pl.pallas_call(
        body,
        out_shape=(
            jax.ShapeDtypeStruct((STATE, 2, ENV), F32),
            jax.ShapeDtypeStruct((ITERS, ENV), F32),
        ),
        in_specs=[pl.BlockSpec(memory_space=pltpu.HBM)] * 11,
        out_specs=(vmem, vmem),
        scratch_shapes=scratch(),
        compiler_params=pltpu.CompilerParams(collective_id=0, has_side_effects=True, vmem_limit_bytes=67043328),
        name="parareal",
    )(init_state, jnp.swapaxes(torque, 0, 1), contact, jnp.swapaxes(mass_inverse, 0, 1), *params, jnp.asarray(PICK, BF16), jnp.asarray(PICK.transpose(0, 2, 1), BF16))
    return jnp.swapaxes(final, 0, 1), corrections


def solution(mesh):
    torus = Mesh(mesh.devices.reshape(NX, NZ, NC, NE), ("x", "z", "c", "e"))
    return jax.shard_map(
        shards,
        mesh=torus,
        in_specs=(
            P(None, "e"),
            P(TM, None, "e"),
            P(TM, "e"),
            P(TM, None, None),
            P(),
            P(),
            P(),
            P(),
            P(),
        ),
        out_specs=(P(TM, None, "e"), P(None, "e")),
        check_vma=False,
    )
```

```python
import math

import jax
import jax.numpy as jnp
import numpy as np
from jax import lax
from jax.experimental import pallas as pl
from jax.experimental.pallas import tpu as pltpu
from jax.sharding import Mesh
from jax.sharding import PartitionSpec as P

DOF = 35
STATE = 70
SUB = 32
ITERS = 3
SWEEPS = ITERS + 1
NX, NZ, NC, NE = 4, 8, 2, 4
GROUP = NZ * NC
ENV = 256
BLOCK = ENV // GROUP
LANES = 128
HALF = 64
MROWS = 80
NROWS = 40
DT = 0.05
H = DT / SUB
TWO_PI = 2.0 * math.pi
F32 = jnp.float32
BF16 = jnp.bfloat16
MESH = pl.DeviceIdType.MESH
HIGHEST = lax.Precision.HIGHEST
TM = ("x", "z", "c")
Z_OFFSETS = (4, 3, 5, 2, 6, 1, 7, 0)
NEAR_FIRST = ((0, 1, 7, 2), (6, 3, 5, 4))
NEAR_CHIPS = (1, 7, 2, 6, 3, 5, 4)


def sine_coefficients(terms):
    x = np.cos(np.linspace(0, np.pi, 4001)) * 0.25 + 0.25
    x = x[x > 1e-4]
    basis = np.stack([x ** (2 * i + 1) for i in range(terms)], 1)
    target = np.sin(2 * np.pi * x)
    weight = np.ones_like(x)
    for _ in range(200):
        c = np.linalg.lstsq(basis * weight[:, None], target * weight, rcond=None)[0]
        weight = weight * (1e-12 + np.abs(basis @ c - target)) ** 0.1
        weight /= weight.mean()
    return [float(np.float32(v)) for v in c]


SINE = sine_coefficients(6)


def selectors():
    pick = np.zeros((2, 2 * LANES, LANES), np.float32)
    for s in range(2):
        for i in range(DOF):
            pick[s, HALF * s + i, i] = 1.0
            pick[s, LANES + HALF * s + i, DOF + i] = 1.0
    return pick


PICK = selectors()


def split(x):
    hi = x.astype(BF16)
    lo = (x - hi.astype(F32)).astype(BF16)
    return hi, lo


def split3(x):
    hi = x.astype(BF16)
    rest = x - hi.astype(F32)
    mid = rest.astype(BF16)
    return hi, mid, (rest - mid.astype(F32)).astype(BF16)


def dot(a, b):
    return jnp.dot(a, b, preferred_element_type=F32)


def exact(a, b):
    return jnp.dot(a, b, precision=HIGHEST, preferred_element_type=F32)


def exact_ta(a, b):
    return lax.dot_general(a, b, (((0,), (0,)), ((), ())), precision=HIGHEST, preferred_element_type=F32)


def exact_tb(a, b):
    return lax.dot_general(a, b, (((1,), (1,)), ((), ())), precision=HIGHEST, preferred_element_type=F32)


def wide(x, weights):
    hi, lo = split(x)
    return dot(hi, weights[0]) + dot(lo, weights[0]) + dot(hi, weights[1])


def pick_right(x, pick):
    hi, mid, lo = split3(x)
    return dot(hi, pick) + dot(mid, pick) + dot(lo, pick)


def pick_left(pick, x):
    hi, mid, lo = split3(x)
    return dot(pick, hi) + dot(pick, mid) + dot(pick, lo)


def put_pair(ref, value):
    hi, lo = split(value)
    ref[0] = hi
    ref[1] = lo


def put_side(ref, index, value):
    hi, lo = split(value)
    ref[index, 0:MROWS, 0:LANES] = hi
    ref[index, 0:MROWS, LANES:] = lo


def small(x, weights):
    rows = x.shape[0]
    hi, lo = split(x)
    out = dot(jnp.concatenate([hi, lo], axis=0), weights)
    both = out[:, 0:LANES] + out[:, LANES:]
    return both[0:rows] + both[rows:]


def body(
    init_in, torque_in, contact_in, minv_in, stiff_in, damp_in, grav_in, cstiff_in, cdamp_in, pick_in, turn_in,
    final_ref, corr_out_ref,
    init_ref, torque_ref, contact_ref, minv_ref, stiff_ref, damp_ref, grav_ref, cstiff_ref, cdamp_ref, pick_ref, turn_ref,
    in_sem, par_ref, block_ref, flip, tau, kk, dd, q_ref, v_ref, init_t, nfine, free, jall, start, gee, ends, jshift, map0_ref,
    mf_w, zf_w, ze_w, s_buf, recv_s, n_buf, recv_n, m_buf, recv_m, side_n, side_a, side_b, side_p, side_pp, side_c,
    prod, lead_ref, ent, total_buf, recv_t, c_buf, recv_c, e_send, recv_e, cnt_buf, recv_cnt,
    corr, recv_cz, corr_x, recv_cx,
    sem_cnt, rsem_cnt, sem_n, rsem_n, sem_m, rsem_m, sem_p, rsem_p, sem_s, rsem_s, sem_e, rsem_e, sem_t, rsem_t, sem_c, rsem_c,
    sem_cz, rsem_cz, sem_cx, rsem_cx,
):
    x, z, c, e = (lax.axis_index(name) for name in ("x", "z", "c", "e"))
    me = z * NC + c

    def zc_peers():
        for dz in Z_OFFSETS:
            for dc in (1, 0):
                if dz == 0 and dc == 0:
                    continue
                pz, pc = lax.rem(z + dz, NZ), lax.rem(c + dc, NC)
                yield pz * NC + pc, {"z": pz, "c": pc}

    def chips(offsets):
        for dz in offsets:
            pz = lax.rem(z + dz, NZ)
            yield pz, {"z": pz}

    def copy(src, dst, ssem, rsem, device):
        return pltpu.make_async_remote_copy(
            src_ref=src, dst_ref=dst, send_sem=ssem, recv_sem=rsem, device_id=device, device_id_type=MESH
        )

    sources = (
        contact_in, minv_in, stiff_in, damp_in, grav_in, cstiff_in, cdamp_in, init_in, torque_in, pick_in, turn_in,
    )
    targets = (
        contact_ref, minv_ref, stiff_ref, damp_ref, grav_ref, cstiff_ref, cdamp_ref,
        init_ref, torque_ref, pick_ref, turn_ref,
    )
    loads = [pltpu.make_async_copy(a, b, in_sem.at[i]) for i, (a, b) in enumerate(zip(sources, targets))]
    for load in loads:
        load.start()
    barrier = pltpu.get_barrier_semaphore()
    for _, device in zc_peers():
        pl.semaphore_signal(barrier, inc=1, device_id=device, device_id_type=MESH)
    for k in range(1, NX):
        pl.semaphore_signal(barrier, inc=1, device_id={"x": lax.rem(x + k, NX)}, device_id_type=MESH)
    for k in range(1, NE):
        pl.semaphore_signal(barrier, inc=1, device_id={"e": lax.rem(e + k, NE)}, device_id_type=MESH)

    for side in (side_a, side_b, side_p, side_pp, side_c, side_n):
        side[...] = jnp.zeros_like(side)
    for load in loads:
        load.wait()
    contact = contact_ref[...].astype(F32)
    counts = jnp.sum(contact, axis=1, keepdims=True)
    cnt_buf[...] = jnp.zeros_like(cnt_buf)
    cnt_buf[0:4, :] = jnp.broadcast_to(counts, (4, LANES))
    lane = lax.broadcasted_iota(jnp.int32, (8, LANES), 1)
    row = lax.broadcasted_iota(jnp.int32, (8, LANES), 0)
    par_ref[...] = jnp.zeros_like(par_ref)
    for i, ref in enumerate((stiff_ref, damp_ref, grav_ref, cstiff_ref, cdamp_ref)):
        par_ref[i : i + 1, 0:DOF] = ref[...]
    par_one = par_ref[...]
    par_ref[...] = par_one + pltpu.roll(par_one, HALF, 1)
    flip[...] = jnp.zeros_like(flip)
    flip[0:DOF, 0:DOF] = minv_ref[:, 1, :]
    shifted = pltpu.roll(flip[0:NROWS, 0:LANES], HALF, 1)
    flip[0:DOF, 0:DOF] = minv_ref[:, 0, :]
    packed = flip[0:NROWS, 0:LANES] + shifted
    n_buf[...] = packed
    recv_n[z] = packed
    low40 = lax.broadcasted_iota(jnp.int32, (NROWS, LANES), 1) < HALF
    def clear(i, unused):
        block_ref[pl.ds(pl.multiple_of(i * HALF, HALF), HALF), :] = jnp.zeros((HALF, LANES), F32)
        return unused

    lax.fori_loop(0, 2, clear, 0)
    block_ref[0:NROWS, :] = jnp.where(low40, packed, 0.0)
    block_ref[HALF : HALF + NROWS, :] = jnp.where(low40, 0.0, packed)
    pl.semaphore_wait(barrier, GROUP - 1 + NX - 1 + NE - 1)

    count_copies = []
    for k in range(1, NE):
        cp = copy(cnt_buf, recv_cnt.at[e], sem_cnt.at[k], rsem_cnt.at[e], {"e": lax.rem(e + k, NE)})
        cp.start()
        count_copies.append(cp)
    n_copies = []
    for p, device in chips(NEAR_CHIPS):
        cp = copy(n_buf, recv_n.at[z], sem_n.at[p], rsem_n.at[z], device)
        cp.start()
        n_copies.append(cp)

    stiff, damp, grav = par_ref[0:1], par_ref[1:2], par_ref[2:3]
    cstiff, cdamp = par_ref[3:4], par_ref[4:5]
    flip[0:STATE, :] = init_ref[...]
    init_t[...] = jnp.transpose(flip[...])
    flip[...] = jnp.zeros_like(flip)
    flip[0:4, :] = contact
    contact8 = flip[0:8, :]
    for j in range(2):
        mine = row == jnp.where(lane < HALF, j, 2 + j)
        kk[j] = (stiff + exact_ta(contact8, jnp.where(mine, jnp.broadcast_to(cstiff, (8, LANES)), 0.0))) * TWO_PI
        dd[j] = (damp + exact_ta(contact8, jnp.where(mine, jnp.broadcast_to(cdamp, (8, LANES)), 0.0))) * (TWO_PI / H)
    flip[0:8, :] = jnp.zeros((8, ENV), F32)
    for j in range(2):
        flip[0:DOF, :] = torque_ref[:, j, :]
        flip[HALF : HALF + DOF, :] = torque_ref[:, 2 + j, :]
        tau[j] = jnp.transpose(flip[...])
    hi, lo = split(block_ref[...] * (H * H / TWO_PI))
    nfine[0:LANES, 0:LANES] = hi
    nfine[0:LANES, LANES:] = lo
    nfine[LANES:, 0:LANES] = hi
    nfine[LANES:, LANES:] = lo

    sums = cnt_buf[...]
    for k in range(1, NE):
        p = lax.rem(e + k, NE)
        copy(cnt_buf, recv_cnt.at[p], sem_cnt.at[k], rsem_cnt.at[p], {"e": p}).wait_recv()
        sums = sums + recv_cnt[p]
    mean = sums * (1.0 / (ENV * NE))
    m_buf[...] = mean
    recv_m[z] = mean
    m_copies = []
    for p, device in chips(NEAR_CHIPS):
        cp = copy(m_buf, recv_m.at[z], sem_m.at[p], rsem_m.at[z], device)
        cp.start()
        m_copies.append(cp)
    lane1 = lane[0:1]
    springs, frictions = [], []
    for j in range(2):
        m = jnp.where(lane1 < HALF, mean[j : j + 1], mean[2 + j : 3 + j])
        springs.append(stiff + grav + m * cstiff)
        frictions.append(damp + m * cdamp)

    def coarse(q, v, forced):
        for j in range(2):
            force = -(springs[j] * q + frictions[j] * v)
            if forced:
                force = force + tau[j]
            v = v + DT * exact(force, block_ref[...])
            q = q + DT * v
        return q, v

    eye = (
        lax.broadcasted_iota(jnp.int32, (LANES, LANES), 0) == lax.broadcasted_iota(jnp.int32, (LANES, LANES), 1)
    ).astype(F32)
    none = jnp.zeros((LANES, LANES), F32)
    mq, mv = coarse(jnp.concatenate([eye, none], axis=0), jnp.concatenate([none, eye], axis=0), False)
    mf = jnp.concatenate([mq, mv], axis=1)
    put_pair(mf_w, mf)
    map0 = pick_left(turn_ref[0], pick_right(mf, pick_ref[0]))
    map1 = pick_left(turn_ref[1], pick_right(mf, pick_ref[1]))
    hi, lo = split(pick_left(pick_ref[0], map1) + pick_ref[1].astype(F32))
    zf_w[:, 0:LANES] = hi
    zf_w[:, LANES:] = lo
    map0_ref[...] = map0

    fq, fv = coarse(jnp.zeros((ENV, LANES), F32), jnp.zeros((ENV, LANES), F32), True)
    free[:, 0:LANES] = fq
    free[:, LANES:] = fv
    jall[...] = jnp.zeros_like(jall)
    gee[...] = jnp.zeros_like(gee)
    ends[...] = jnp.zeros_like(ends)
    corr[...] = jnp.zeros_like(corr)
    for cp in count_copies:
        cp.wait_send()

    def fine():
        q_ref[...] = start[:, 0:LANES] * (1.0 / TWO_PI)
        v_ref[...] = start[:, LANES:] * (H / TWO_PI)
        coef = [grav * value for value in SINE]

        def horizon(j, unused):
            def substep(counter, unused2):
                q, v = q_ref[...], v_ref[...]
                r = q - jnp.round(q)
                r2 = r * r
                r4 = r2 * r2
                low, mid, high = (coef[i + 1] * r2 + coef[i] for i in (0, 2, 4))
                poly = (high * r4 + mid) * r4 + low
                force = tau[j] - kk[j] * q - dd[j] * v - r * poly
                hi, lo = split(force)
                out = dot(jnp.concatenate([hi, lo], axis=1), nfine[...])
                v = v + (out[:, 0:LANES] + out[:, LANES:])
                v_ref[...] = v
                q_ref[...] = q + v
                return unused2

            return lax.fori_loop(0, SUB, substep, unused, unroll=32)

        lax.fori_loop(0, 2, horizon, 0)
        free[:, 0:LANES] = q_ref[...] * TWO_PI
        free[:, LANES:] = v_ref[...] * (TWO_PI / H)

    def settle(slot):
        new = gee[...] + jall[...]
        change = new - ends[...]
        ends[...] = new
        square = change * change
        folded = square[:, 0:LANES] + square[:, LANES:]
        ones = ((row == 0) & (lane < HALF)) | ((row == 1) & (lane >= HALF))
        ones = ones.astype(F32).astype(BF16)
        sums = None
        for piece in split(folded):
            term = lax.dot_general(ones, piece, (((1,), (1,)), ((), ())), preferred_element_type=F32)
            sums = term if sums is None else sums + term
        largest = jnp.sqrt(jnp.maximum(sums[0:1], sums[1:2]))
        corr[pl.ds(slot, 1), :] = largest[:, 0:LANES]
        corr[pl.ds(slot + 4, 1), :] = largest[:, LANES:]

    def maps(offsets):
        rr = lax.broadcasted_iota(jnp.int32, (MROWS, LANES), 0)
        ll = lax.broadcasted_iota(jnp.int32, (MROWS, LANES), 1)
        base_q = ((rr == ll) & (ll < DOF)).astype(F32)
        base_v = ((rr == ll + DOF) & (ll < DOF)).astype(F32)
        keep = lane[0:1] < HALF
        one = [jnp.where(keep, par_ref[i : i + 1], 0.0) for i in range(5)]
        for p, device in chips([dz for dz in offsets if dz]):
            copy(n_buf, recv_n.at[p], sem_n.at[p], rsem_n.at[p], device).wait_recv()
            copy(m_buf, recv_m.at[p], sem_m.at[p], rsem_m.at[p], device).wait_recv()
        for u, (p, _) in enumerate(chips(offsets)):
            n_both = recv_n[p]
            means = recv_m[p]
            q, v = base_q, base_v
            for s in range(2):
                n_one = jnp.where(low40, pltpu.roll(n_both, HALF, 1) if s else n_both, 0.0)
                hi, lo = split(n_one)
                side_n[2 * u + s, 0:NROWS, 0:LANES] = hi
                side_n[2 * u + s, 0:NROWS, LANES:] = lo
                for j in range(2):
                    m = means[2 * s + j : 2 * s + j + 1]
                    spring = one[0] + one[2] + m * one[3]
                    friction = one[1] + m * one[4]
                    v = v - DT * small(spring * q + friction * v, side_n[2 * u + s])
                    q = q + DT * v
            prod[p * NC + c] = q + pltpu.roll(v, DOF, 1)
        for p, _ in chips(offsets):
            swap(p * NC + c, p).start()

    def swap(slot, p):
        return copy(prod.at[slot], prod.at[slot], sem_p.at[p], rsem_p.at[p], {"c": 1 - c})

    def products():
        for offsets in NEAR_FIRST:
            maps(offsets)
        for p in range(NZ):
            put_side(side_a, p * NC + c, prod[p * NC + c])
        for p in range(NZ):
            swap(p * NC + 1 - c, p).wait_recv()
            put_side(side_a, p * NC + 1 - c, prod[p * NC + 1 - c])
        for i in range(4):
            acc = prod[4 * i]
            for j in range(1, 4):
                put_side(side_p, 4 * i + j, acc)
                acc = small(acc, side_a[4 * i + j])
            put_side(side_b, i, acc)
            lead_ref[i] = acc
            if i == 0:
                before = acc
        leads = [before]
        for i in range(1, 4):
            leads.append(small(leads[-1], side_b[i]))
        c_buf[...] = leads[3]
        for k in range(1, NX):

            @pl.when(x + k < NX)
            def _():
                copy(c_buf, recv_c.at[x], sem_c.at[k], rsem_c.at[x], {"x": lax.rem(x + k, NX)}).start()

        two = small(lead_ref[1], side_b[2])
        put_side(side_b, 4, two)
        put_side(side_b, 5, small(lead_ref[2], side_b[3]))
        put_side(side_b, 6, small(two, side_b[3]))
        for i in range(3):
            lead_ref[i] = leads[i]
        for j in range(1, 4):
            side_pp[j] = side_p[j]
        for i in range(1, 4):
            put_side(side_pp, 4 * i, lead_ref[i - 1])
            for j in range(1, 4):
                put_side(side_pp, 4 * i + j, small(lead_ref[i - 1], side_p[4 * i + j]))

    def place_maps():
        place = turn_ref[0].astype(F32) + pick_right(map0_ref[...], turn_ref[1])
        for part, value in enumerate((place, wide(place, mf_w))):
            hi, lo = split(value)
            cols = slice(2 * LANES * part, 2 * LANES * (part + 1))
            ze_w[0:LANES, cols] = hi
            ze_w[LANES : 2 * LANES, cols] = hi
            ze_w[2 * LANES :, cols] = lo

    def sweep(k, unused):
        @pl.when(k > 0)
        def _():
            fine()

        fresh = free[...] - gee[...]
        hi, lo = split(fresh)
        shifts = dot(hi, zf_w[...]) + dot(lo, zf_w[...])
        s_buf[...] = shifts[:, 0:LANES] + shifts[:, LANES:]
        recv_s[k, me] = s_buf[pl.ds(me * BLOCK, BLOCK), :]
        s_copies = []
        for p, device in zc_peers():
            cp = copy(s_buf.at[pl.ds(p * BLOCK, BLOCK)], recv_s.at[k, me], sem_s.at[p], rsem_s.at[k, me], device)
            cp.start()
            s_copies.append(cp)

        @pl.when(k > 0)
        def _():
            settle(lax.max(k - 2, 0))

        jall[...] = fresh

        @pl.when(k == 0)
        def _():
            products()

        for p, device in zc_peers():
            copy(s_buf.at[pl.ds(0, BLOCK)], recv_s.at[k, p], sem_s.at[p], rsem_s.at[k, p], device).wait_recv()

        inside = {}
        totals = []
        for i in range(4):
            acc = recv_s[k, 4 * i]
            for j in range(1, 4):
                inside[i, j] = acc
                acc = small(acc, side_a[4 * i + j]) + recv_s[k, 4 * i + j]
            totals.append(acc)
        total_buf[...] = (
            small(totals[0], side_b[6]) + small(totals[1], side_b[5]) + small(totals[2], side_b[3]) + totals[3]
        )
        for d in range(1, NX):

            @pl.when(x + d < NX)
            def _():
                copy(total_buf, recv_t.at[k, x], sem_t.at[d], rsem_t.at[k, x], {"x": lax.rem(x + d, NX)}).start()

        entry = [
            None,
            totals[0],
            small(totals[0], side_b[1]) + totals[1],
            small(totals[0], side_b[4]) + small(totals[1], side_b[2]) + totals[2],
        ]
        for i in range(4):
            if i > 0:
                ent[4 * i] = entry[i]
            for j in range(1, 4):
                value = inside[i, j]
                if i > 0:
                    value = small(entry[i], side_p[4 * i + j]) + value
                ent[4 * i + j] = value
        ent[0] = init_t[pl.ds(me * BLOCK, BLOCK), :]
        for d in range(NX - 1):

            @pl.when(x > d)
            def _():
                @pl.when(k == 0)
                def _():
                    copy(c_buf, recv_c.at[d], sem_c.at[d], rsem_c.at[d], {"x": d}).wait_recv()
                    put_side(side_c, d, recv_c[d])

                copy(total_buf, recv_t.at[k, d], sem_t.at[d], rsem_t.at[k, d], {"x": d}).wait_recv()
                ent[0] = small(ent[0], side_c[d]) + recv_t[k, d]

        first = ent[0]
        e_send[0] = first
        for d in range(1, GROUP):
            e_send[d] = small(first, side_pp[d]) + ent[d]
        recv_e[k, me] = e_send[me]
        e_copies = []
        for p, device in zc_peers():
            cp = copy(e_send.at[p], recv_e.at[k, me], sem_e.at[p], rsem_e.at[k, me], device)
            cp.start()
            e_copies.append(cp)

        @pl.when(k == 0)
        def _():
            place_maps()

        low = lax.broadcasted_iota(jnp.int32, (ENV, LANES), 1) < HALF
        for part in range(2):
            cols = slice(part * LANES, (part + 1) * LANES)
            jshift[:, cols] = jnp.where(low, 0.0, pltpu.roll(jall[:, cols], HALF, 1))
        jshift[:, 2 * LANES :] = wide(jshift[:, 0 : 2 * LANES], mf_w)
        for p, device in zc_peers():
            copy(e_send.at[p], recv_e.at[k, p], sem_e.at[p], rsem_e.at[k, p], device).wait_recv()

        arrived = recv_e[k].reshape(ENV, LANES)
        hi, lo = split(arrived)
        both = dot(jnp.concatenate([hi, lo], axis=1), ze_w[0 : 2 * LANES, :]) + dot(hi, ze_w[2 * LANES :, :])
        start[...] = both[:, 0 : 2 * LANES] + jshift[:, 0 : 2 * LANES]
        gee[...] = both[:, 2 * LANES :] + jshift[:, 2 * LANES :]
        for cp in s_copies:
            cp.wait_send()
        for cp in e_copies:
            cp.wait_send()
        for d in range(1, NX):

            @pl.when(x + d < NX)
            def _():
                copy(total_buf, recv_t.at[k, x], sem_t.at[d], rsem_t.at[k, x], {"x": lax.rem(x + d, NX)}).wait_send()

        return unused

    lax.fori_loop(0, SWEEPS, sweep, 0)

    settle(ITERS - 1)
    cz_copies = []
    recv_cz[me] = corr[...]
    for p, device in zc_peers():
        cp = copy(corr, recv_cz.at[me], sem_cz.at[p], rsem_cz.at[me], device)
        cp.start()
        cz_copies.append(cp)
    for s in range(2):
        final_ref[:, s, :] = lax.dot_general(
            pick_ref[s].astype(F32), ends[...], (((0,), (1,)), ((), ())), precision=HIGHEST, preferred_element_type=F32
        )[0:STATE]
    for p, device in zc_peers():
        copy(corr, recv_cz.at[p], sem_cz.at[p], rsem_cz.at[p], device).wait_recv()
    corr_x[...] = jnp.max(recv_cz[...], axis=0)
    cx_copies = []
    for d in range(1, NX):
        cp = copy(corr_x, recv_cx.at[x], sem_cx.at[d], rsem_cx.at[x], {"x": lax.rem(x + d, NX)})
        cp.start()
        cx_copies.append(cp)
    best = corr_x[...]
    for d in range(1, NX):
        p = lax.rem(x + d, NX)
        copy(corr_x, recv_cx.at[p], sem_cx.at[d], rsem_cx.at[p], {"x": p}).wait_recv()
        best = jnp.maximum(best, recv_cx[p])
    corr_out_ref[:, 0:LANES] = best[0:ITERS]
    corr_out_ref[:, LANES:] = best[4 : 4 + ITERS]
    for p in range(NZ):
        swap(p * NC + c, p).wait_send()
    for cp in n_copies + m_copies + cz_copies + cx_copies:
        cp.wait_send()
    for k in range(1, NX):

        @pl.when(x + k < NX)
        def _():
            copy(c_buf, recv_c.at[x], sem_c.at[k], rsem_c.at[x], {"x": lax.rem(x + k, NX)}).wait_send()


def scratch():
    def v(*shape, dtype=F32):
        return pltpu.VMEM(shape, dtype)

    dma = pltpu.SemaphoreType.DMA
    return [
        v(STATE, ENV),
        v(DOF, 4, ENV),
        pltpu.VMEM((4, ENV), jnp.int32),
        v(DOF, 2, DOF),
        *[v(1, DOF) for _ in range(5)],
        v(2, 2 * LANES, LANES, dtype=BF16),
        v(2, LANES, 2 * LANES, dtype=BF16),
        dma((11,)),
        v(8, LANES),
        v(LANES, LANES),
        v(LANES, ENV),
        v(2, ENV, LANES),
        v(2, ENV, LANES),
        v(2, ENV, LANES),
        v(ENV, LANES),
        v(ENV, LANES),
        v(ENV, LANES),
        v(2 * LANES, 2 * LANES, dtype=BF16),
        v(ENV, 2 * LANES),
        v(ENV, 2 * LANES),
        v(ENV, 2 * LANES),
        v(ENV, 2 * LANES),
        v(ENV, 2 * LANES),
        v(ENV, 4 * LANES),
        v(LANES, LANES),
        v(2, 2 * LANES, 2 * LANES, dtype=BF16),
        v(2 * LANES, 2 * LANES, dtype=BF16),
        v(3 * LANES, 4 * LANES, dtype=BF16),
        v(ENV, LANES),
        v(SWEEPS, GROUP, BLOCK, LANES),
        v(NROWS, LANES),
        v(NZ, NROWS, LANES),
        v(8, LANES),
        v(NZ, 8, LANES),
        v(8, LANES, 2 * LANES, dtype=BF16),
        v(GROUP, LANES, 2 * LANES, dtype=BF16),
        v(7, LANES, 2 * LANES, dtype=BF16),
        v(GROUP, LANES, 2 * LANES, dtype=BF16),
        v(GROUP, LANES, 2 * LANES, dtype=BF16),
        v(NX, LANES, 2 * LANES, dtype=BF16),
        v(GROUP, MROWS, LANES),
        v(4, MROWS, LANES),
        v(GROUP, BLOCK, LANES),
        v(BLOCK, LANES),
        v(SWEEPS, NX, BLOCK, LANES),
        v(MROWS, LANES),
        v(NX, MROWS, LANES),
        v(GROUP, BLOCK, LANES),
        v(SWEEPS, GROUP, BLOCK, LANES),
        v(8, LANES),
        v(NE, 8, LANES),
        v(8, LANES),
        v(GROUP, 8, LANES),
        v(8, LANES),
        v(NX, 8, LANES),
        dma((NE,)), dma((NE,)),
        dma((NZ,)), dma((NZ,)),
        dma((NZ,)), dma((NZ,)),
        dma((NZ,)), dma((NZ,)),
        dma((GROUP,)), dma((SWEEPS, GROUP)),
        dma((GROUP,)), dma((SWEEPS, GROUP)),
        dma((NX,)), dma((SWEEPS, NX)),
        dma((NX,)), dma((NX,)),
        dma((GROUP,)), dma((GROUP,)),
        dma((NX,)), dma((NX,)),
    ]


def shards(
    init_state, torque, contact, mass_inverse, stiffness, damping, gravity, contact_stiffness, contact_damping
):
    params = [p.reshape(1, DOF) for p in (stiffness, damping, gravity, contact_stiffness, contact_damping)]
    vmem = pl.BlockSpec(memory_space=pltpu.VMEM)
    final, corrections = pl.pallas_call(
        body,
        out_shape=(
            jax.ShapeDtypeStruct((STATE, 2, ENV), F32),
            jax.ShapeDtypeStruct((ITERS, ENV), F32),
        ),
        in_specs=[pl.BlockSpec(memory_space=pltpu.HBM)] * 11,
        out_specs=(vmem, vmem),
        scratch_shapes=scratch(),
        compiler_params=pltpu.CompilerParams(collective_id=0, has_side_effects=True, vmem_limit_bytes=67043328),
        name="parareal",
    )(init_state, jnp.swapaxes(torque, 0, 1), contact, jnp.swapaxes(mass_inverse, 0, 1), *params, jnp.asarray(PICK, BF16), jnp.asarray(PICK.transpose(0, 2, 1), BF16))
    return jnp.swapaxes(final, 0, 1), corrections


def solution(mesh):
    torus = Mesh(mesh.devices.reshape(NX, NZ, NC, NE), ("x", "z", "c", "e"))
    return jax.shard_map(
        shards,
        mesh=torus,
        in_specs=(
            P(None, "e"),
            P(TM, None, "e"),
            P(TM, "e"),
            P(TM, None, None),
            P(),
            P(),
            P(),
            P(),
            P(),
        ),
        out_specs=(P(TM, None, "e"), P(None, "e")),
        check_vma=False,
    )
```

```python
import math

import jax
import jax.numpy as jnp
import numpy as np
from jax import lax
from jax.experimental import pallas as pl
from jax.experimental.pallas import tpu as pltpu
from jax.sharding import Mesh
from jax.sharding import PartitionSpec as P

DOF = 35
STATE = 70
SUB = 32
ITERS = 3
SWEEPS = ITERS + 1
NX, NZ, NC, NE = 4, 8, 2, 4
GROUP = NZ * NC
ENV = 256
BLOCK = ENV // GROUP
LANES = 128
HALF = 64
MROWS = 80
NROWS = 40
DT = 0.05
H = DT / SUB
TWO_PI = 2.0 * math.pi
F32 = jnp.float32
BF16 = jnp.bfloat16
MESH = pl.DeviceIdType.MESH
HIGHEST = lax.Precision.HIGHEST
TM = ("x", "z", "c")
Z_OFFSETS = (4, 3, 5, 2, 6, 1, 7, 0)
NEAR_FIRST = ((0, 1, 7, 2), (6, 3, 5, 4))
NEAR_CHIPS = (1, 7, 2, 6, 3, 5, 4)


def sine_coefficients(terms):
    x = np.cos(np.linspace(0, np.pi, 4001)) * 0.25 + 0.25
    x = x[x > 1e-4]
    basis = np.stack([x ** (2 * i + 1) for i in range(terms)], 1)
    target = np.sin(2 * np.pi * x)
    weight = np.ones_like(x)
    for _ in range(200):
        c = np.linalg.lstsq(basis * weight[:, None], target * weight, rcond=None)[0]
        weight = weight * (1e-12 + np.abs(basis @ c - target)) ** 0.1
        weight /= weight.mean()
    return [float(np.float32(v)) for v in c]


SINE = sine_coefficients(6)


def selectors():
    pick = np.zeros((2, 2 * LANES, LANES), np.float32)
    for s in range(2):
        for i in range(DOF):
            pick[s, HALF * s + i, i] = 1.0
            pick[s, LANES + HALF * s + i, DOF + i] = 1.0
    return pick


PICK = selectors()


def split(x):
    hi = x.astype(BF16)
    lo = (x - hi.astype(F32)).astype(BF16)
    return hi, lo


def split3(x):
    hi = x.astype(BF16)
    rest = x - hi.astype(F32)
    mid = rest.astype(BF16)
    return hi, mid, (rest - mid.astype(F32)).astype(BF16)


def dot(a, b):
    return jnp.dot(a, b, preferred_element_type=F32)


def exact(a, b):
    return jnp.dot(a, b, precision=HIGHEST, preferred_element_type=F32)


def exact_ta(a, b):
    return lax.dot_general(a, b, (((0,), (0,)), ((), ())), precision=HIGHEST, preferred_element_type=F32)


def exact_tb(a, b):
    return lax.dot_general(a, b, (((1,), (1,)), ((), ())), precision=HIGHEST, preferred_element_type=F32)


def wide(x, weights):
    hi, lo = split(x)
    return dot(hi, weights[0]) + dot(lo, weights[0]) + dot(hi, weights[1])


def pick_right(x, pick):
    hi, mid, lo = split3(x)
    return dot(hi, pick) + dot(mid, pick) + dot(lo, pick)


def pick_left(pick, x):
    hi, mid, lo = split3(x)
    return dot(pick, hi) + dot(pick, mid) + dot(pick, lo)


def put_pair(ref, value):
    hi, lo = split(value)
    ref[0] = hi
    ref[1] = lo


def put_side(ref, index, value):
    hi, lo = split(value)
    ref[index, 0:MROWS, 0:LANES] = hi
    ref[index, 0:MROWS, LANES:] = lo


def small(x, weights):
    rows = x.shape[0]
    hi, lo = split(x)
    out = dot(jnp.concatenate([hi, lo], axis=0), weights)
    both = out[:, 0:LANES] + out[:, LANES:]
    return both[0:rows] + both[rows:]


def body(
    init_in, torque_in, contact_in, minv_in, stiff_in, damp_in, grav_in, cstiff_in, cdamp_in, pick_in, turn_in,
    final_ref, corr_out_ref,
    init_ref, torque_ref, contact_ref, minv_ref, stiff_ref, damp_ref, grav_ref, cstiff_ref, cdamp_ref, pick_ref, turn_ref,
    in_sem, par_ref, block_ref, flip, tau, kk, dd, q_ref, v_ref, init_t, nfine, free, jall, start, gee, ends, jshift, map0_ref,
    mf_w, zf_w, ze_w, s_buf, recv_s, n_buf, recv_n, m_buf, recv_m, side_n, side_a, side_b, side_p, side_pp, side_c,
    prod, lead_ref, ent, total_buf, recv_t, c_buf, recv_c, e_send, recv_e, cnt_buf, recv_cnt,
    corr, recv_cz, corr_x, recv_cx,
    sem_cnt, rsem_cnt, sem_n, rsem_n, sem_m, rsem_m, sem_p, rsem_p, sem_s, rsem_s, sem_e, rsem_e, sem_t, rsem_t, sem_c, rsem_c,
    sem_cz, rsem_cz, sem_cx, rsem_cx,
):
    x, z, c, e = (lax.axis_index(name) for name in ("x", "z", "c", "e"))
    me = z * NC + c

    def zc_peers():
        for dz in Z_OFFSETS:
            for dc in (1, 0):
                if dz == 0 and dc == 0:
                    continue
                pz, pc = lax.rem(z + dz, NZ), lax.rem(c + dc, NC)
                yield pz * NC + pc, {"z": pz, "c": pc}

    def chips(offsets):
        for dz in offsets:
            pz = lax.rem(z + dz, NZ)
            yield pz, {"z": pz}

    def copy(src, dst, ssem, rsem, device):
        return pltpu.make_async_remote_copy(
            src_ref=src, dst_ref=dst, send_sem=ssem, recv_sem=rsem, device_id=device, device_id_type=MESH
        )

    sources = (
        contact_in, minv_in, stiff_in, damp_in, grav_in, cstiff_in, cdamp_in, init_in, torque_in, pick_in, turn_in,
    )
    targets = (
        contact_ref, minv_ref, stiff_ref, damp_ref, grav_ref, cstiff_ref, cdamp_ref,
        init_ref, torque_ref, pick_ref, turn_ref,
    )
    loads = [pltpu.make_async_copy(a, b, in_sem.at[i]) for i, (a, b) in enumerate(zip(sources, targets))]
    for load in loads:
        load.start()
    barrier = pltpu.get_barrier_semaphore()
    for _, device in zc_peers():
        pl.semaphore_signal(barrier, inc=1, device_id=device, device_id_type=MESH)
    for k in range(1, NX):
        pl.semaphore_signal(barrier, inc=1, device_id={"x": lax.rem(x + k, NX)}, device_id_type=MESH)
    for k in range(1, NE):
        pl.semaphore_signal(barrier, inc=1, device_id={"e": lax.rem(e + k, NE)}, device_id_type=MESH)

    for side in (side_a, side_b, side_p, side_pp, side_c, side_n):
        side[...] = jnp.zeros_like(side)
    for load in loads:
        load.wait()
    contact = contact_ref[...].astype(F32)
    counts = jnp.sum(contact, axis=1, keepdims=True)
    cnt_buf[...] = jnp.zeros_like(cnt_buf)
    cnt_buf[0:4, :] = jnp.broadcast_to(counts, (4, LANES))
    lane = lax.broadcasted_iota(jnp.int32, (8, LANES), 1)
    row = lax.broadcasted_iota(jnp.int32, (8, LANES), 0)
    par_ref[...] = jnp.zeros_like(par_ref)
    for i, ref in enumerate((stiff_ref, damp_ref, grav_ref, cstiff_ref, cdamp_ref)):
        par_ref[i : i + 1, 0:DOF] = ref[...]
    par_one = par_ref[...]
    par_ref[...] = par_one + pltpu.roll(par_one, HALF, 1)
    flip[...] = jnp.zeros_like(flip)
    flip[0:DOF, 0:DOF] = minv_ref[:, 1, :]
    shifted = pltpu.roll(flip[0:NROWS, 0:LANES], HALF, 1)
    flip[0:DOF, 0:DOF] = minv_ref[:, 0, :]
    packed = flip[0:NROWS, 0:LANES] + shifted
    n_buf[...] = packed
    recv_n[z] = packed
    low40 = lax.broadcasted_iota(jnp.int32, (NROWS, LANES), 1) < HALF
    def clear(i, unused):
        block_ref[pl.ds(pl.multiple_of(i * HALF, HALF), HALF), :] = jnp.zeros((HALF, LANES), F32)
        return unused

    lax.fori_loop(0, 2, clear, 0)
    block_ref[0:NROWS, :] = jnp.where(low40, packed, 0.0)
    block_ref[HALF : HALF + NROWS, :] = jnp.where(low40, 0.0, packed)
    pl.semaphore_wait(barrier, GROUP - 1 + NX - 1 + NE - 1)

    count_copies = []
    for k in range(1, NE):
        cp = copy(cnt_buf, recv_cnt.at[e], sem_cnt.at[k], rsem_cnt.at[e], {"e": lax.rem(e + k, NE)})
        cp.start()
        count_copies.append(cp)
    n_copies = []
    for p, device in chips(NEAR_CHIPS):
        cp = copy(n_buf, recv_n.at[z], sem_n.at[p], rsem_n.at[z], device)
        cp.start()
        n_copies.append(cp)

    stiff, damp, grav = par_ref[0:1], par_ref[1:2], par_ref[2:3]
    cstiff, cdamp = par_ref[3:4], par_ref[4:5]
    flip[0:STATE, :] = init_ref[...]
    init_t[...] = jnp.transpose(flip[...])
    flip[...] = jnp.zeros_like(flip)
    flip[0:4, :] = contact
    contact8 = flip[0:8, :]
    for j in range(2):
        mine = row == jnp.where(lane < HALF, j, 2 + j)
        kk[j] = (stiff + exact_ta(contact8, jnp.where(mine, jnp.broadcast_to(cstiff, (8, LANES)), 0.0))) * TWO_PI
        dd[j] = (damp + exact_ta(contact8, jnp.where(mine, jnp.broadcast_to(cdamp, (8, LANES)), 0.0))) * (TWO_PI / H)
    flip[0:8, :] = jnp.zeros((8, ENV), F32)
    for j in range(2):
        flip[0:DOF, :] = torque_ref[:, j, :]
        flip[HALF : HALF + DOF, :] = torque_ref[:, 2 + j, :]
        tau[j] = jnp.transpose(flip[...])
    hi, lo = split(block_ref[...] * (H * H / TWO_PI))
    nfine[0:LANES, 0:LANES] = hi
    nfine[0:LANES, LANES:] = lo
    nfine[LANES:, 0:LANES] = hi
    nfine[LANES:, LANES:] = lo

    sums = cnt_buf[...]
    for k in range(1, NE):
        p = lax.rem(e + k, NE)
        copy(cnt_buf, recv_cnt.at[p], sem_cnt.at[k], rsem_cnt.at[p], {"e": p}).wait_recv()
        sums = sums + recv_cnt[p]
    mean = sums * (1.0 / (ENV * NE))
    m_buf[...] = mean
    recv_m[z] = mean
    m_copies = []
    for p, device in chips(NEAR_CHIPS):
        cp = copy(m_buf, recv_m.at[z], sem_m.at[p], rsem_m.at[z], device)
        cp.start()
        m_copies.append(cp)
    lane1 = lane[0:1]
    springs, frictions = [], []
    for j in range(2):
        m = jnp.where(lane1 < HALF, mean[j : j + 1], mean[2 + j : 3 + j])
        springs.append(stiff + grav + m * cstiff)
        frictions.append(damp + m * cdamp)

    def coarse(q, v, forced):
        for j in range(2):
            force = -(springs[j] * q + frictions[j] * v)
            if forced:
                force = force + tau[j]
            v = v + DT * exact(force, block_ref[...])
            q = q + DT * v
        return q, v

    eye = (
        lax.broadcasted_iota(jnp.int32, (LANES, LANES), 0) == lax.broadcasted_iota(jnp.int32, (LANES, LANES), 1)
    ).astype(F32)
    none = jnp.zeros((LANES, LANES), F32)
    mq, mv = coarse(jnp.concatenate([eye, none], axis=0), jnp.concatenate([none, eye], axis=0), False)
    mf = jnp.concatenate([mq, mv], axis=1)
    put_pair(mf_w, mf)
    map0 = pick_left(turn_ref[0], pick_right(mf, pick_ref[0]))
    map1 = pick_left(turn_ref[1], pick_right(mf, pick_ref[1]))
    hi, lo = split(pick_left(pick_ref[0], map1) + pick_ref[1].astype(F32))
    zf_w[:, 0:LANES] = hi
    zf_w[:, LANES:] = lo
    map0_ref[...] = map0

    fq, fv = coarse(jnp.zeros((ENV, LANES), F32), jnp.zeros((ENV, LANES), F32), True)
    free[:, 0:LANES] = fq
    free[:, LANES:] = fv
    jall[...] = jnp.zeros_like(jall)
    gee[...] = jnp.zeros_like(gee)
    ends[...] = jnp.zeros_like(ends)
    corr[...] = jnp.zeros_like(corr)
    for cp in count_copies:
        cp.wait_send()

    def fine():
        q_ref[...] = start[:, 0:LANES] * (1.0 / TWO_PI)
        v_ref[...] = start[:, LANES:] * (H / TWO_PI)
        coef = [grav * value for value in SINE]

        def horizon(j, unused):
            def substep(counter, unused2):
                q, v = q_ref[...], v_ref[...]
                r = q - jnp.round(q)
                r2 = r * r
                r4 = r2 * r2
                low, mid, high = (coef[i + 1] * r2 + coef[i] for i in (0, 2, 4))
                poly = (high * r4 + mid) * r4 + low
                force = tau[j] - kk[j] * q - dd[j] * v - r * poly
                hi, lo = split(force)
                out = dot(jnp.concatenate([hi, lo], axis=1), nfine[...])
                v = v + (out[:, 0:LANES] + out[:, LANES:])
                v_ref[...] = v
                q_ref[...] = q + v
                return unused2

            return lax.fori_loop(0, SUB, substep, unused, unroll=32)

        lax.fori_loop(0, 2, horizon, 0)
        free[:, 0:LANES] = q_ref[...] * TWO_PI
        free[:, LANES:] = v_ref[...] * (TWO_PI / H)

    def settle(slot):
        new = gee[...] + jall[...]
        change = new - ends[...]
        ends[...] = new
        square = change * change
        folded = square[:, 0:LANES] + square[:, LANES:]
        ones = ((row == 0) & (lane < HALF)) | ((row == 1) & (lane >= HALF))
        ones = ones.astype(F32).astype(BF16)
        sums = None
        for piece in split(folded):
            term = lax.dot_general(ones, piece, (((1,), (1,)), ((), ())), preferred_element_type=F32)
            sums = term if sums is None else sums + term
        largest = jnp.sqrt(jnp.maximum(sums[0:1], sums[1:2]))
        corr[pl.ds(slot, 1), :] = largest[:, 0:LANES]
        corr[pl.ds(slot + 4, 1), :] = largest[:, LANES:]

    def maps(offsets):
        rr = lax.broadcasted_iota(jnp.int32, (MROWS, LANES), 0)
        ll = lax.broadcasted_iota(jnp.int32, (MROWS, LANES), 1)
        base_q = ((rr == ll) & (ll < DOF)).astype(F32)
        base_v = ((rr == ll + DOF) & (ll < DOF)).astype(F32)
        keep = lane[0:1] < HALF
        one = [jnp.where(keep, par_ref[i : i + 1], 0.0) for i in range(5)]
        for p, device in chips([dz for dz in offsets if dz]):
            copy(n_buf, recv_n.at[p], sem_n.at[p], rsem_n.at[p], device).wait_recv()
            copy(m_buf, recv_m.at[p], sem_m.at[p], rsem_m.at[p], device).wait_recv()
        for u, (p, _) in enumerate(chips(offsets)):
            n_both = recv_n[p]
            means = recv_m[p]
            q, v = base_q, base_v
            for s in range(2):
                n_one = jnp.where(low40, pltpu.roll(n_both, HALF, 1) if s else n_both, 0.0)
                hi, lo = split(n_one)
                side_n[2 * u + s, 0:NROWS, 0:LANES] = hi
                side_n[2 * u + s, 0:NROWS, LANES:] = lo
                for j in range(2):
                    m = means[2 * s + j : 2 * s + j + 1]
                    spring = one[0] + one[2] + m * one[3]
                    friction = one[1] + m * one[4]
                    v = v - DT * small(spring * q + friction * v, side_n[2 * u + s])
                    q = q + DT * v
            prod[p * NC + c] = q + pltpu.roll(v, DOF, 1)
        for p, _ in chips(offsets):
            swap(p * NC + c, p).start()

    def swap(slot, p):
        return copy(prod.at[slot], prod.at[slot], sem_p.at[p], rsem_p.at[p], {"c": 1 - c})

    def products():
        for offsets in NEAR_FIRST:
            maps(offsets)
        for p in range(NZ):
            put_side(side_a, p * NC + c, prod[p * NC + c])
        for p in range(NZ):
            swap(p * NC + 1 - c, p).wait_recv()
            put_side(side_a, p * NC + 1 - c, prod[p * NC + 1 - c])
        for i in range(4):
            acc = prod[4 * i]
            for j in range(1, 4):
                put_side(side_p, 4 * i + j, acc)
                acc = small(acc, side_a[4 * i + j])
            put_side(side_b, i, acc)
            lead_ref[i] = acc
            if i == 0:
                before = acc
        leads = [before]
        for i in range(1, 4):
            leads.append(small(leads[-1], side_b[i]))
        c_buf[...] = leads[3]
        for k in range(1, NX):

            @pl.when(x + k < NX)
            def _():
                copy(c_buf, recv_c.at[x], sem_c.at[k], rsem_c.at[x], {"x": lax.rem(x + k, NX)}).start()

        two = small(lead_ref[1], side_b[2])
        put_side(side_b, 4, two)
        put_side(side_b, 5, small(lead_ref[2], side_b[3]))
        put_side(side_b, 6, small(two, side_b[3]))
        for i in range(3):
            lead_ref[i] = leads[i]
        for j in range(1, 4):
            side_pp[j] = side_p[j]
        for i in range(1, 4):
            put_side(side_pp, 4 * i, lead_ref[i - 1])
            for j in range(1, 4):
                put_side(side_pp, 4 * i + j, small(lead_ref[i - 1], side_p[4 * i + j]))

    def place_maps():
        place = turn_ref[0].astype(F32) + pick_right(map0_ref[...], turn_ref[1])
        for part, value in enumerate((place, wide(place, mf_w))):
            hi, lo = split(value)
            cols = slice(2 * LANES * part, 2 * LANES * (part + 1))
            ze_w[0:LANES, cols] = hi
            ze_w[LANES : 2 * LANES, cols] = hi
            ze_w[2 * LANES :, cols] = lo

    def sent(k):
        for p, device in zc_peers():
            copy(e_send.at[p], recv_e.at[k - 1, me], sem_e.at[p], rsem_e.at[k - 1, me], device).wait_send()
        for d in range(1, NX):

            @pl.when(x + d < NX)
            def _():
                device = {"x": lax.rem(x + d, NX)}
                copy(total_buf, recv_t.at[k - 1, x], sem_t.at[d], rsem_t.at[k - 1, x], device).wait_send()

    def sweep(k, unused):
        @pl.when(k > 0)
        def _():
            fine()

        fresh = free[...] - gee[...]
        hi, lo = split(fresh)
        shifts = dot(hi, zf_w[...]) + dot(lo, zf_w[...])
        s_buf[...] = shifts[:, 0:LANES] + shifts[:, LANES:]
        recv_s[k, me] = s_buf[pl.ds(me * BLOCK, BLOCK), :]
        s_copies = []
        for p, device in zc_peers():
            cp = copy(s_buf.at[pl.ds(p * BLOCK, BLOCK)], recv_s.at[k, me], sem_s.at[p], rsem_s.at[k, me], device)
            cp.start()
            s_copies.append(cp)

        @pl.when(k > 0)
        def _():
            sent(k)
            settle(lax.max(k - 2, 0))

        jall[...] = fresh

        @pl.when(k == 0)
        def _():
            products()

        for p, device in zc_peers():
            copy(s_buf.at[pl.ds(0, BLOCK)], recv_s.at[k, p], sem_s.at[p], rsem_s.at[k, p], device).wait_recv()

        inside = {}
        totals = []
        for i in range(4):
            acc = recv_s[k, 4 * i]
            for j in range(1, 4):
                inside[i, j] = acc
                acc = small(acc, side_a[4 * i + j]) + recv_s[k, 4 * i + j]
            totals.append(acc)
        total_buf[...] = (
            small(totals[0], side_b[6]) + small(totals[1], side_b[5]) + small(totals[2], side_b[3]) + totals[3]
        )
        for d in range(1, NX):

            @pl.when(x + d < NX)
            def _():
                copy(total_buf, recv_t.at[k, x], sem_t.at[d], rsem_t.at[k, x], {"x": lax.rem(x + d, NX)}).start()

        entry = [
            None,
            totals[0],
            small(totals[0], side_b[1]) + totals[1],
            small(totals[0], side_b[4]) + small(totals[1], side_b[2]) + totals[2],
        ]
        for i in range(4):
            if i > 0:
                ent[4 * i] = entry[i]
            for j in range(1, 4):
                value = inside[i, j]
                if i > 0:
                    value = small(entry[i], side_p[4 * i + j]) + value
                ent[4 * i + j] = value
        ent[0] = init_t[pl.ds(me * BLOCK, BLOCK), :]
        for d in range(NX - 1):

            @pl.when(x > d)
            def _():
                @pl.when(k == 0)
                def _():
                    copy(c_buf, recv_c.at[d], sem_c.at[d], rsem_c.at[d], {"x": d}).wait_recv()
                    put_side(side_c, d, recv_c[d])

                copy(total_buf, recv_t.at[k, d], sem_t.at[d], rsem_t.at[k, d], {"x": d}).wait_recv()
                ent[0] = small(ent[0], side_c[d]) + recv_t[k, d]

        first = ent[0]
        e_send[0] = first
        for d in range(1, GROUP):
            e_send[d] = small(first, side_pp[d]) + ent[d]
        recv_e[k, me] = e_send[me]
        for p, device in zc_peers():
            copy(e_send.at[p], recv_e.at[k, me], sem_e.at[p], rsem_e.at[k, me], device).start()
        for cp in s_copies:
            cp.wait_send()

        @pl.when(k == 0)
        def _():
            place_maps()

        low = lax.broadcasted_iota(jnp.int32, (ENV, LANES), 1) < HALF
        for part in range(2):
            cols = slice(part * LANES, (part + 1) * LANES)
            jshift[:, cols] = jnp.where(low, 0.0, pltpu.roll(jall[:, cols], HALF, 1))
        jshift[:, 2 * LANES :] = wide(jshift[:, 0 : 2 * LANES], mf_w)
        for p, device in zc_peers():
            copy(e_send.at[p], recv_e.at[k, p], sem_e.at[p], rsem_e.at[k, p], device).wait_recv()

        arrived = recv_e[k].reshape(ENV, LANES)
        hi, lo = split(arrived)
        both = dot(jnp.concatenate([hi, lo], axis=1), ze_w[0 : 2 * LANES, :]) + dot(hi, ze_w[2 * LANES :, :])
        start[...] = both[:, 0 : 2 * LANES] + jshift[:, 0 : 2 * LANES]
        gee[...] = both[:, 2 * LANES :] + jshift[:, 2 * LANES :]
        return unused

    lax.fori_loop(0, SWEEPS, sweep, 0)

    settle(ITERS - 1)
    cz_copies = []
    recv_cz[me] = corr[...]
    for p, device in zc_peers():
        cp = copy(corr, recv_cz.at[me], sem_cz.at[p], rsem_cz.at[me], device)
        cp.start()
        cz_copies.append(cp)
    for s in range(2):
        final_ref[:, s, :] = lax.dot_general(
            pick_ref[s].astype(F32), ends[...], (((0,), (1,)), ((), ())), precision=HIGHEST, preferred_element_type=F32
        )[0:STATE]
    sent(SWEEPS)
    for p, device in zc_peers():
        copy(corr, recv_cz.at[p], sem_cz.at[p], rsem_cz.at[p], device).wait_recv()
    corr_x[...] = jnp.max(recv_cz[...], axis=0)
    cx_copies = []
    for d in range(1, NX):
        cp = copy(corr_x, recv_cx.at[x], sem_cx.at[d], rsem_cx.at[x], {"x": lax.rem(x + d, NX)})
        cp.start()
        cx_copies.append(cp)
    best = corr_x[...]
    for d in range(1, NX):
        p = lax.rem(x + d, NX)
        copy(corr_x, recv_cx.at[p], sem_cx.at[d], rsem_cx.at[p], {"x": p}).wait_recv()
        best = jnp.maximum(best, recv_cx[p])
    corr_out_ref[:, 0:LANES] = best[0:ITERS]
    corr_out_ref[:, LANES:] = best[4 : 4 + ITERS]
    for p in range(NZ):
        swap(p * NC + c, p).wait_send()
    for cp in n_copies + m_copies + cz_copies + cx_copies:
        cp.wait_send()
    for k in range(1, NX):

        @pl.when(x + k < NX)
        def _():
            copy(c_buf, recv_c.at[x], sem_c.at[k], rsem_c.at[x], {"x": lax.rem(x + k, NX)}).wait_send()


def scratch():
    def v(*shape, dtype=F32):
        return pltpu.VMEM(shape, dtype)

    dma = pltpu.SemaphoreType.DMA
    return [
        v(STATE, ENV),
        v(DOF, 4, ENV),
        pltpu.VMEM((4, ENV), jnp.int32),
        v(DOF, 2, DOF),
        *[v(1, DOF) for _ in range(5)],
        v(2, 2 * LANES, LANES, dtype=BF16),
        v(2, LANES, 2 * LANES, dtype=BF16),
        dma((11,)),
        v(8, LANES),
        v(LANES, LANES),
        v(LANES, ENV),
        v(2, ENV, LANES),
        v(2, ENV, LANES),
        v(2, ENV, LANES),
        v(ENV, LANES),
        v(ENV, LANES),
        v(ENV, LANES),
        v(2 * LANES, 2 * LANES, dtype=BF16),
        v(ENV, 2 * LANES),
        v(ENV, 2 * LANES),
        v(ENV, 2 * LANES),
        v(ENV, 2 * LANES),
        v(ENV, 2 * LANES),
        v(ENV, 4 * LANES),
        v(LANES, LANES),
        v(2, 2 * LANES, 2 * LANES, dtype=BF16),
        v(2 * LANES, 2 * LANES, dtype=BF16),
        v(3 * LANES, 4 * LANES, dtype=BF16),
        v(ENV, LANES),
        v(SWEEPS, GROUP, BLOCK, LANES),
        v(NROWS, LANES),
        v(NZ, NROWS, LANES),
        v(8, LANES),
        v(NZ, 8, LANES),
        v(8, LANES, 2 * LANES, dtype=BF16),
        v(GROUP, LANES, 2 * LANES, dtype=BF16),
        v(7, LANES, 2 * LANES, dtype=BF16),
        v(GROUP, LANES, 2 * LANES, dtype=BF16),
        v(GROUP, LANES, 2 * LANES, dtype=BF16),
        v(NX, LANES, 2 * LANES, dtype=BF16),
        v(GROUP, MROWS, LANES),
        v(4, MROWS, LANES),
        v(GROUP, BLOCK, LANES),
        v(BLOCK, LANES),
        v(SWEEPS, NX, BLOCK, LANES),
        v(MROWS, LANES),
        v(NX, MROWS, LANES),
        v(GROUP, BLOCK, LANES),
        v(SWEEPS, GROUP, BLOCK, LANES),
        v(8, LANES),
        v(NE, 8, LANES),
        v(8, LANES),
        v(GROUP, 8, LANES),
        v(8, LANES),
        v(NX, 8, LANES),
        dma((NE,)), dma((NE,)),
        dma((NZ,)), dma((NZ,)),
        dma((NZ,)), dma((NZ,)),
        dma((NZ,)), dma((NZ,)),
        dma((GROUP,)), dma((SWEEPS, GROUP)),
        dma((GROUP,)), dma((SWEEPS, GROUP)),
        dma((NX,)), dma((SWEEPS, NX)),
        dma((NX,)), dma((NX,)),
        dma((GROUP,)), dma((GROUP,)),
        dma((NX,)), dma((NX,)),
    ]


def shards(
    init_state, torque, contact, mass_inverse, stiffness, damping, gravity, contact_stiffness, contact_damping
):
    params = [p.reshape(1, DOF) for p in (stiffness, damping, gravity, contact_stiffness, contact_damping)]
    vmem = pl.BlockSpec(memory_space=pltpu.VMEM)
    final, corrections = pl.pallas_call(
        body,
        out_shape=(
            jax.ShapeDtypeStruct((STATE, 2, ENV), F32),
            jax.ShapeDtypeStruct((ITERS, ENV), F32),
        ),
        in_specs=[pl.BlockSpec(memory_space=pltpu.HBM)] * 11,
        out_specs=(vmem, vmem),
        scratch_shapes=scratch(),
        compiler_params=pltpu.CompilerParams(collective_id=0, has_side_effects=True, vmem_limit_bytes=67043328),
        name="parareal",
    )(init_state, jnp.swapaxes(torque, 0, 1), contact, jnp.swapaxes(mass_inverse, 0, 1), *params, jnp.asarray(PICK, BF16), jnp.asarray(PICK.transpose(0, 2, 1), BF16))
    return jnp.swapaxes(final, 0, 1), corrections


def solution(mesh):
    torus = Mesh(mesh.devices.reshape(NX, NZ, NC, NE), ("x", "z", "c", "e"))
    return jax.shard_map(
        shards,
        mesh=torus,
        in_specs=(
            P(None, "e"),
            P(TM, None, "e"),
            P(TM, "e"),
            P(TM, None, None),
            P(),
            P(),
            P(),
            P(),
            P(),
        ),
        out_specs=(P(TM, None, "e"), P(None, "e")),
        check_vma=False,
    )
```
